256 devices in a mesh: bins: 16 (over x, z_lo, core), sta: 16 (over z_hi, y).
Axes of the slice: x: 4, y: 4, z: 8 (z_hi: 4, z_lo: 2; z = z_hi * 2 + z_lo), core: 2. Of those that a mesh axis runs over, the one named last changes fastest.
Arguments:
- spectra: bfloat16 [2, 128, 8, 4096], P(None, 'bins', None, 'sta'), may hold values from -110 to 110
- coords: int32 [2, 4096], replicated, may hold values from 0 to 2047
- slowness: int32 [2, 2048], replicated, may hold values from -32 to 31
Outputs:
- beam_power: float32 [128, 2048], P('bins', 'sta')
The draws below stay inside these ranges and needn't reach their ends.
All inputs are finite; a program needn't handle non-finite values.
Results may differ from the reference program's by a relative error of at most 0.002.
Values may be sent and summed in bfloat16 or wider, within the bound.
A program may use at most 64 MiB of HBM per device.

```python
import math
import jax
import jax.numpy as jnp
from jax import lax

FREQS = 128
BEAMS = 2048
SEGS = 8
STATIONS = 4096


def draw_spectra(key, part):
    keys = jax.random.split(key, 3)
    levels = jnp.arange(FREQS, dtype=jnp.float32) / FREQS
    tilt = jnp.exp(jnp.log(4.0) * levels)
    seg_gain = jax.random.uniform(keys[1], (SEGS,), jnp.float32, 0.5, 1.5)
    noise = jnp.clip(jax.random.normal(keys[0], (2, FREQS, SEGS, STATIONS), jnp.float32), -3.0, 3.0)
    station_gain = jnp.exp(jax.random.uniform(keys[2], (STATIONS,), jnp.float32, jnp.log(0.5), jnp.log(2.0)))
    values = noise * tilt[None, :, None, None] * seg_gain[None, None, :, None] * station_gain[None, None, None, :]
    return values.astype(jnp.bfloat16)


def plant(entries, key, least, top_value):
    spot = [jax.random.randint(jax.random.fold_in(key, axis), (), 0, length) for axis, length in enumerate(entries.shape)]
    widest = entries.shape.index(max(entries.shape))
    next_to = spot[:widest] + [(spot[widest] + 1) % entries.shape[widest]] + spot[widest + 1:]
    return entries.at[tuple(spot)].set(least).at[tuple(next_to)].set(top_value)


def setup_inputs(seed: int = 0) -> dict:
    seeds = jax.random.split(jax.random.key(seed), 4)
    spectra = draw_spectra(jax.random.fold_in(seeds[3], 71), 0)
    coords = plant(jax.random.randint(seeds[1], (2, STATIONS), 0, 2048), jax.random.fold_in(seeds[1], 1), 0, 2047).astype(jnp.int32)
    slowness = plant(jax.random.randint(seeds[2], (2, BEAMS), -32, 32), jax.random.fold_in(seeds[2], 1), -32, 31).astype(jnp.int32)
    return {"spectra": spectra, "coords": coords, "slowness": slowness}


phase_modulus = 1048576
two_pi = 2.0 * math.pi
epsilon = 1e-06

def steering_table(delays, bin_number):
    phase_index = jnp.mod(bin_number * delays, phase_modulus)
    phase = phase_index.astype(jnp.float32) * (two_pi / phase_modulus)
    return jnp.concatenate([jnp.cos(phase), jnp.sin(phase)], 0).astype(jnp.bfloat16)

def reference(spectra, coords, slowness):
    values = spectra.astype(jnp.float32)
    sumsq = lax.optimization_barrier(jnp.sum(values * values, axis=(0, 1)))
    scale = jnp.sqrt(sumsq / (2 * FREQS) + epsilon)
    whitened = (values / scale).astype(jnp.bfloat16)
    delays = slowness[0][None, :] * coords[0][:, None] + slowness[1][None, :] * coords[1][:, None]

    def one_bin(pair_args):
        bin_white, bin_number = pair_args
        real_part = bin_white[0]
        imag_part = bin_white[1]
        upper_rows = jnp.concatenate([real_part, imag_part], 1)
        bottom = jnp.concatenate([imag_part, -imag_part * 0 - real_part], 1)
        stacked = jnp.concatenate([upper_rows, bottom], 0).astype(jnp.float32)
        steering = steering_table(delays, bin_number).astype(jnp.float32)
        amplitude = jnp.dot(stacked, steering, preferred_element_type=jnp.float32)
        return lax.optimization_barrier(jnp.sum(amplitude * amplitude, axis=0))
    bin_numbers = jnp.arange(1, FREQS + 1, dtype=jnp.int32)
    beam_power = lax.map(one_bin, (jnp.moveaxis(whitened, 1, 0), bin_numbers))
    return beam_power / (STATIONS * SEGS)
```

```python
import math

import jax
import jax.numpy as jnp
import numpy as np
from jax import lax
from jax.experimental import pallas as pl
from jax.experimental.pallas import tpu as pltpu
from jax.sharding import PartitionSpec as P

MESH = pl.DeviceIdType.MESH
epsilon = 1e-06
GRID_K = 32
N_BINS = 16
N_STA = 16


def cheb_fit(fn, degree):
    nodes = np.cos(np.pi * (np.arange(4001) + 0.5) / 4001)
    u = (nodes + 1.0) / 2.0
    return np.polynomial.chebyshev.Chebyshev.fit(u, fn(u), degree, domain=[0, 1]).convert(
        kind=np.polynomial.Polynomial
    ).coef


def cos_coefs():
    return [float(c) for c in cheb_fit(lambda u: np.cos(np.pi * np.sqrt(u)), 7)]


def sin_coefs():
    return [float(c) for c in cheb_fit(lambda u: np.pi * np.sinc(np.sqrt(u)), 6)]


COS = cos_coefs()
SIN = sin_coefs()


def horner(coefs, u):
    acc = jnp.full_like(u, coefs[-1])
    for c in coefs[-2::-1]:
        acc = acc * u + c
    return acc


def cos_sin(index):
    t = lax.shift_right_arithmetic(lax.shift_left(index, 11), 11).astype(jnp.float32) * (1.0 / 1048576)
    u = t * t
    return horner(COS, u), horner(SIN, u) * t


def kernel(
    x_hbm, co_hbm, sl_hbm, out_ref,
    xv, cov, slv, raw_send, raw_recv, part_send, part_recv, r_send, r_recv, pow_send, pow_recv,
    tabx, taby, xrot, wbuf, pick,
    in_sem, part_ss, part_rs, raw_ss, raw_rs, r_ss, r_rs, pow_ss, pow_rs,
):
    bi = lax.axis_index("bins")
    sj = lax.axis_index("sta")
    core = bi % 2
    chip = bi - core
    half = sj % 2
    f1 = bi * 8 + sj // 2 + 1

    loads = [
        pltpu.make_async_copy(src, dst, in_sem.at[n])
        for n, (src, dst) in enumerate(((x_hbm, xv), (co_hbm, cov), (sl_hbm, slv)))
    ]
    for load in loads:
        load.start()

    barrier = pltpu.get_barrier_semaphore()

    def greet_bins(d, _):
        pl.semaphore_signal(barrier, inc=1, device_id=((bi + d) % N_BINS, sj), device_id_type=MESH)
        return 0

    def greet_sta(d, _):
        q = (sj + d) % N_STA
        pl.semaphore_signal(barrier, inc=1, device_id=(bi, q), device_id_type=MESH)
        pl.semaphore_signal(barrier, inc=1, device_id=(chip + 1 - core, q), device_id_type=MESH)
        return 0

    lax.fori_loop(1, N_BINS, greet_bins, 0)
    lax.fori_loop(1, N_STA, greet_sta, 0)

    loads[0].wait()
    sq = jnp.zeros((8, 256), jnp.float32)
    for b in range(8):
        re = xv[0, b].astype(jnp.float32)
        im = xv[1, b].astype(jnp.float32)
        sq = sq + (re * re + im * im)
        for h in range(2):
            rows = slice(4 * h, 4 * h + 4)
            raw_send[2 * b + h] = jnp.concatenate(
                [re[rows, :128], im[rows, :128], re[rows, 128:], im[rows, 128:]], 0
            ).astype(jnp.bfloat16)
    for h in range(2):
        rows = slice(4 * h, 4 * h + 4)
        part_send[h] = jnp.concatenate([sq[rows, :128], sq[rows, 128:]], 0)

    pl.semaphore_wait(barrier, 45)

    def part_copy(d):
        p = (bi + d) % N_BINS
        return pltpu.make_async_remote_copy(
            src_ref=part_send.at[p % 2], dst_ref=part_recv.at[bi],
            send_sem=part_ss.at[p], recv_sem=part_rs.at[bi],
            device_id=(p, sj), device_id_type=MESH,
        )

    def raw_copy(d):
        q = (sj + d) % N_STA
        return pltpu.make_async_remote_copy(
            src_ref=raw_send.at[q], dst_ref=raw_recv.at[sj],
            send_sem=raw_ss.at[q], recv_sem=raw_rs.at[sj],
            device_id=(bi, q), device_id_type=MESH,
        )

    def r_copy(dc, e):
        q = ((sj // 2 + e) % 8) * 2 + core
        return pltpu.make_async_remote_copy(
            src_ref=r_send, dst_ref=r_recv.at[sj],
            send_sem=r_ss.at[dc * 8 + e], recv_sem=r_rs.at[sj],
            device_id=(chip + (core + dc) % 2, q), device_id_type=MESH,
        )

    def pow_copy(d):
        q = (sj + d) % N_STA
        return pltpu.make_async_remote_copy(
            src_ref=pow_send.at[q], dst_ref=pow_recv.at[sj],
            send_sem=pow_ss.at[q], recv_sem=pow_rs.at[sj],
            device_id=(bi, q), device_id_type=MESH,
        )

    def arrival(buf, sems, k):
        return pltpu.make_async_copy(buf.at[k], buf.at[k], sems.at[k])

    def loop(lo, hi, body):
        lax.fori_loop(lo, hi, lambda d, c: (body(d), c)[1], 0)

    loop(1, N_BINS, lambda d: part_copy(d).start())
    loop(1, N_STA, lambda d: raw_copy(d).start())
    part_recv[bi] = part_send[core]
    raw_recv[sj] = raw_send[sj]

    loads[1].wait()
    loads[2].wait()
    odd = lax.broadcasted_iota(jnp.int32, (GRID_K, 256), 0) * 2 + 1

    def tables(j):
        lanes = pl.ds(pl.multiple_of(j * 256, 256), 256)
        cx = cov[0:1, lanes] * f1
        cy = cov[1:2, lanes] * f1
        c, s = cos_sin(odd * cx)
        tabx[0, :, lanes] = c
        tabx[1, :, lanes] = s
        c, s = cos_sin(odd * cy)
        c = c.astype(jnp.bfloat16)
        s = s.astype(jnp.bfloat16)
        taby[:, lanes] = jnp.concatenate([c, c, s, s], 0)

    loop(0, 16, tables)

    def part_wait(d):
        p = (bi + d) % N_BINS
        arrival(part_recv, part_rs, p).wait()

    loop(1, N_BINS, part_wait)
    total = part_recv[0]
    for p in range(1, N_BINS):
        total = total + part_recv[p]
    inv = 1.0 / jnp.sqrt(total / 256.0 + epsilon)
    r_send[...] = inv
    loop(0, 8, lambda e: r_copy(1, e).start())
    loop(1, 8, lambda e: r_copy(0, e).start())

    @pl.when(half != core)
    def _():
        r_copy(0, 0).start()

    @pl.when(half == core)
    def _():
        r_recv[sj] = inv

    sx = slv[0:1, :]
    sy = slv[1:2, :]
    xneg = lax.shift_right_arithmetic(sx, 31)
    yneg = lax.shift_right_arithmetic(sy, 31)
    kx = sx ^ xneg
    ky = sy ^ yneg
    quad = jnp.where(sx >= 0, jnp.where(sy >= 0, 0, 32), jnp.where(sy >= 0, 96, 64))
    where_y = ky + quad
    for n in range(0, 2048, 256):
        hot = lax.broadcasted_iota(jnp.int32, (128, 256), 0) == where_y[:, n : n + 256]
        pick[:, n : n + 256] = jnp.where(hot, 1.0, 0.0).astype(jnp.bfloat16)

    loop(1, N_STA, lambda d: arrival(raw_recv, raw_rs, (sj + d) % N_STA).wait())
    sign = jnp.where(lax.broadcasted_iota(jnp.int32, (8, 256), 0) < 4, -1.0, 1.0)

    def rotate(j):
        lanes = pl.ds(pl.multiple_of(j * 256, 256), 256)
        raw = raw_recv[j].astype(jnp.float32)
        x = jnp.concatenate([raw[:8], raw[8:]], 1)
        swapped = jnp.concatenate([x[4:], x[:4]], 0)
        both = (cov[0:1, lanes] + cov[1:2, lanes]) * f1
        c, s = cos_sin(jnp.broadcast_to(both, (8, 256)))
        xrot[:, lanes] = x * c + swapped * (s * sign)

    loop(0, 16, rotate)

    loop(1, N_STA, lambda d: arrival(r_recv, r_rs, (sj + d) % N_STA).wait())

    @pl.when(half != core)
    def _():
        arrival(r_recv, r_rs, sj).wait()

    acc = None
    for j in range(16):
        lanes = slice(j * 256, j * 256 + 256)
        r = r_recv[j]
        scale = jnp.concatenate(
            [jnp.concatenate([r[:4], r[:4]], 0), jnp.concatenate([r[4:], r[4:]], 0)], 1
        )
        wbuf[:, lanes] = xrot[:, lanes] * scale
        cosx = tabx[0, :, lanes]
        sinx = tabx[1, :, lanes]
        rows = []
        for part in range(2):
            for tab in (cosx, sinx):
                for g in range(4):
                    n = part * 4 + g
                    rows.append((wbuf[n : n + 1, lanes] * tab).astype(jnp.bfloat16))
        v = jnp.concatenate(rows, 0)
        term = lax.dot_general(
            v, taby[:, lanes], (((1,), (1,)), ((), ())), preferred_element_type=jnp.float32
        )
        acc = term if acc is None else acc + term

    lane = lax.broadcasted_iota(jnp.int32, (128, 128), 1)
    m1 = jnp.where(lane < 96, 1.0, -1.0)
    m2 = jnp.where(lane < 32, -1.0, 1.0)
    re = acc[:128] * m1 + pltpu.roll(acc[128:256], 64, 1) * m2
    im = pltpu.roll(acc[256:384] * m1 + pltpu.roll(acc[384:], 64, 1) * m2, 64, 1)
    plus = (re + im) * (re + im)
    minus = (re - im) * (re - im)
    plus = (plus[:32] + plus[32:64]) + (plus[64:96] + plus[96:])
    minus = (minus[:32] + minus[32:64]) + (minus[64:96] + minus[96:])
    grid = plus + pltpu.roll(minus, 64, 1)
    high = grid.astype(jnp.bfloat16)
    low = (grid - high.astype(jnp.float32)).astype(jnp.bfloat16)
    parts = jnp.concatenate([high, low], 0)
    for n in range(0, 2048, 256):
        picked = jnp.dot(parts, pick[:, n : n + 256], preferred_element_type=jnp.float32)
        picked = picked[:32] + picked[32:]
        hot = lax.broadcasted_iota(jnp.int32, (GRID_K, 256), 0) == kx[:, n : n + 256]
        res = jnp.sum(jnp.where(hot, picked, 0.0), 0, keepdims=True)
        pow_send[n // 128] = res[:, :128]
        pow_send[n // 128 + 1] = res[:, 128:]

    loop(1, N_STA, lambda d: pow_copy(d).start())
    pow_recv[sj] = pow_send[sj]
    loop(1, N_STA, lambda d: arrival(pow_recv, pow_rs, (sj + d) % N_STA).wait())
    for b in range(8):
        out_ref[b : b + 1, :] = (pow_recv[2 * b] + pow_recv[2 * b + 1]) * (1.0 / 32768)

    loop(1, N_BINS, lambda d: part_copy(d).wait_send())
    loop(1, N_STA, lambda d: raw_copy(d).wait_send())
    loop(0, 8, lambda e: r_copy(1, e).wait_send())
    loop(1, 8, lambda e: r_copy(0, e).wait_send())

    @pl.when(half != core)
    def _():
        r_copy(0, 0).wait_send()

    loop(1, N_STA, lambda d: pow_copy(d).wait_send())


def local(spectra, coords, slowness):
    f32, bf16, i32 = jnp.float32, jnp.bfloat16, jnp.int32
    dma = pltpu.SemaphoreType.DMA
    return pl.pallas_call(
        kernel,
        out_shape=jax.ShapeDtypeStruct((8, 128), f32),
        in_specs=[pl.BlockSpec(memory_space=pl.ANY)] * 3,
        out_specs=pl.BlockSpec(memory_space=pltpu.VMEM),
        scratch_shapes=[
            pltpu.VMEM((2, 8, 8, 256), bf16),
            pltpu.VMEM((2, 4096), i32),
            pltpu.VMEM((2, 2048), i32),
            pltpu.VMEM((16, 16, 128), bf16),
            pltpu.VMEM((16, 16, 128), bf16),
            pltpu.VMEM((2, 8, 128), f32),
            pltpu.VMEM((16, 8, 128), f32),
            pltpu.VMEM((8, 128), f32),
            pltpu.VMEM((16, 8, 128), f32),
            pltpu.VMEM((16, 1, 128), f32),
            pltpu.VMEM((16, 1, 128), f32),
            pltpu.VMEM((2, GRID_K, 4096), f32),
            pltpu.VMEM((128, 4096), bf16),
            pltpu.VMEM((8, 4096), f32),
            pltpu.VMEM((8, 4096), f32),
            pltpu.VMEM((128, 2048), bf16),
            dma((3,)),
            dma((16,)), dma((16,)), dma((16,)), dma((16,)),
            dma((16,)), dma((16,)), dma((16,)), dma((16,)),
        ],
        compiler_params=pltpu.CompilerParams(collective_id=0, has_side_effects=True),
    )(spectra, coords, slowness)


def solution(mesh):
    in_specs = (P(None, "bins", None, "sta"), P(), P())
    out_specs = P("bins", "sta")
    return jax.shard_map(local, mesh=mesh, in_specs=in_specs, out_specs=out_specs, check_vma=False)
```

```python
import jax
import jax.numpy as jnp
import numpy as np
from jax import lax
from jax.experimental import pallas as pl
from jax.experimental.pallas import tpu as pltpu
from jax.sharding import PartitionSpec as P

MESH = pl.DeviceIdType.MESH
epsilon = 1e-06
scope = jax.named_scope

GROUPS = (
    ((0, 0), (0, 1), (0, 3), (0, 2)),
    ((1, 0), (3, 0), (1, 1), (3, 3)),
    ((1, 3), (3, 1), (1, 2), (3, 2)),
    ((2, 0), (2, 1), (2, 3), (2, 2)),
)
FAR = [(o, g) for g in range(3, -1, -1) for o in GROUPS[g][::-1]]
FAR_BINS = sorted(((dx, dl) for dx in range(4) for dl in range(2)), key=lambda o: -min(o[0], 4 - o[0]) - o[1])


def cheb_fit(fn, degree):
    nodes = np.cos(np.pi * (np.arange(4001) + 0.5) / 4001)
    u = (nodes + 1.0) / 2.0
    return np.polynomial.chebyshev.Chebyshev.fit(u, fn(u), degree, domain=[0, 1]).convert(
        kind=np.polynomial.Polynomial
    ).coef


COS = [float(c) for c in cheb_fit(lambda u: np.cos(np.pi * np.sqrt(u)), 7)]
SIN = [float(c) for c in cheb_fit(lambda u: np.pi * np.sinc(np.sqrt(u)), 6)]


def horner(coefs, u):
    acc = jnp.full_like(u, coefs[-1])
    for c in coefs[-2::-1]:
        acc = acc * u + c
    return acc


def cos_sin(index):
    t = lax.shift_right_arithmetic(lax.shift_left(index, 11), 11).astype(jnp.float32) * (1.0 / 1048576)
    u = t * t
    return horner(COS, u), horner(SIN, u) * t


def iota(shape, dim):
    return lax.broadcasted_iota(jnp.int32, shape, dim)


def kernel(
    x_hbm, co_hbm, sl_hbm, out_ref,
    xv, cov, slv, raw_send, raw_recv, part_send, part_recv, tot_send, tot_recv, pow_send, pow_recv,
    tabc, tabt, tabr, xrot, wbuf, accum,
    in_sem, part_ss, part_rs, raw_ss, raw_rs, tot_ss, tot_rs, pow_ss, pow_rs,
):
    bi = lax.axis_index("bins")
    sj = lax.axis_index("sta")
    core = lax.rem(bi, 2)
    chip = bi - core
    px = lax.div(bi, 4)
    pl_lo = lax.rem(lax.div(bi, 2), 2)
    pz = lax.div(sj, 4)
    py = lax.rem(sj, 4)
    pair = lax.div(sj, 8)
    own = lax.rem(sj, 8)
    f1 = bi * 8 + own + 1

    def sta_at(o):
        return lax.rem(pz + o[0], 4) * 4 + lax.rem(py + o[1], 4)

    def chip_at(o):
        return lax.rem(px + o[0], 4) * 4 + lax.rem(pl_lo + o[1], 2) * 2

    loads = [
        pltpu.make_async_copy(src, dst, in_sem.at[n])
        for n, (src, dst) in enumerate(((x_hbm, xv), (co_hbm, cov), (sl_hbm, slv)))
    ]
    for load in loads:
        load.start()

    barrier = pltpu.get_barrier_semaphore()

    def greet(b, s):
        pl.semaphore_signal(barrier, inc=1, device_id=(b, s), device_id_type=MESH)

    def loop(lo, hi, body):
        lax.fori_loop(lo, hi, lambda d, c: (body(d), c)[1], 0)

    with scope("a_greet"):
        @pl.when(core == 1)
        def _():
            for o in FAR_BINS:
                greet(chip_at(o), sj)
                if o != (0, 0):
                    greet(chip_at(o) + 1, sj)

        @pl.when(core == 0)
        def _():
            loop(0, 16, lambda d: greet(chip + 1, lax.rem(sj + d, 16)))

        loop(1, 16, lambda d: greet(bi, lax.rem(sj + d, 16)))

    with scope("b_xwait"):
        loads[0].wait()

    with scope("c_sumsq"):
        sq = jnp.zeros((8, 256), jnp.float32)
        for b in range(8):
            re = xv[0, b].astype(jnp.float32)
            im = xv[1, b].astype(jnp.float32)
            sq = sq + (re * re + im * im)
            raw_send[b] = jnp.concatenate(
                [re[:, :128], im[:, :128], re[:, 128:], im[:, 128:]], 0
            ).astype(jnp.bfloat16)
        part = jnp.concatenate([sq[:, :128], sq[:, 128:]], 0).astype(jnp.bfloat16)
        part_send[...] = part

    with scope("d_barrier"):
        @pl.when(core == 1)
        def _():
            pl.semaphore_wait(barrier, 38)

        @pl.when(core == 0)
        def _():
            pl.semaphore_wait(barrier, 23)

    def part_copy(n):
        return pltpu.make_async_remote_copy(
            src_ref=part_send, dst_ref=part_recv.at[bi],
            send_sem=part_ss, recv_sem=part_rs,
            device_id=(chip_at(FAR_BINS[n]) + 1, sj), device_id_type=MESH,
        )

    def raw_copy(n):
        q = sta_at(FAR[n][0])
        return pltpu.make_async_remote_copy(
            src_ref=raw_send.at[lax.rem(q, 8)], dst_ref=raw_recv.at[sj],
            send_sem=raw_ss, recv_sem=raw_rs,
            device_id=(bi, q), device_id_type=MESH,
        )

    def tot_copy(n, c):
        return pltpu.make_async_remote_copy(
            src_ref=tot_send, dst_ref=tot_recv.at[sj],
            send_sem=tot_ss.at[c], recv_sem=tot_rs.at[FAR[n][1]],
            device_id=(chip + c, sta_at(FAR[n][0])), device_id_type=MESH,
        )

    def pow_copy(d):
        m = lax.rem(own + d, 8)
        return pltpu.make_async_remote_copy(
            src_ref=pow_send.at[m], dst_ref=pow_recv.at[own],
            send_sem=pow_ss, recv_sem=pow_rs,
            device_id=(bi, pair * 8 + m), device_id_type=MESH,
        )

    def wait_all(buf, count, sem):
        blocks = buf.at[pl.ds(0, count)]
        pltpu.make_async_copy(blocks, blocks, sem).wait()

    with scope("e_send1"):
        for n in range(7):
            part_copy(n).start()

        @pl.when(core == 0)
        def _():
            part_copy(7).start()

        @pl.when(core == 1)
        def _():
            part_recv[bi] = part

        for n in range(15):
            raw_copy(n).start()
        raw_recv[sj] = raw_send[own]

    loads[1].wait()
    loads[2].wait()
    row8 = iota((8, 256), 0)
    odd32 = iota((32, 256), 0) * 2 + 1
    coarse = row8 * 8 + 4
    fine = jnp.where(row8 == 0, 1, 3)

    def tables(j):
        lanes = pl.ds(pl.multiple_of(j * 256, 256), 256)
        cx = cov[0:1, lanes] * f1
        cy = cov[1:2, lanes] * f1
        c, s = cos_sin(coarse * cx)
        tabc[0, :, lanes] = c
        tabc[1, :, lanes] = s
        c, s = cos_sin(jnp.where(row8 < 2, fine * cx, jnp.broadcast_to(cx + cy, (8, 256))))
        tabr[0, :, lanes] = c
        tabr[1, :, lanes] = s
        cyt, syt = cos_sin(odd32 * cy)
        cols = []
        for trig in range(2):
            for tab in (cyt, syt):
                for f in range(2):
                    cols.append(tabr[trig, f : f + 1, lanes] * tab)
        tabt[lanes, :] = jnp.concatenate(cols, 0).astype(jnp.bfloat16).T

    with scope("f_tables"):
        loop(0, 16, tables)

    @pl.when(core == 1)
    def _():
        with scope("g_partwait"):
            wait_all(part_recv, 15, part_rs)
        with scope("h_total"):
            total = part_recv[0].astype(jnp.float32)
            for p in range(1, 16):
                total = total + part_recv[p].astype(jnp.float32)
            total = total.astype(jnp.bfloat16)
            tot_send[...] = total
            for n in range(15):
                tot_copy(n, 0).start()
                tot_copy(n, 1).start()
            tot_copy(15, 0).start()
            tot_recv[sj] = total

    with scope("i_pick"):
        beams = pl.ds(pl.multiple_of(pair * 1024, 1024), 1024)
        sx = slv[0:1, beams]
        sy = slv[1:2, beams]
        u = sx + 32
        m = lax.shift_right_arithmetic(u, 2)
        f = u & 3
        cpos = m >= 8
        fpos = f >= 2
        ypos = sy >= 0
        cidx = jnp.where(cpos, m - 8, 7 - m)
        fidx = jnp.where(fpos, f - 2, 1 - f)
        ky = jnp.where(ypos, sy, -1 - sy)
        c01 = jnp.where(cpos, 1, 0)
        rel = jnp.where(c01 == jnp.where(fpos, 1, 0), 0, 1)
        diff = jnp.where(c01 == jnp.where(ypos, 1, 0), 0, 1)
        pick_row = (rel * 2 + diff) * 8 + cidx
        pick_col = (1 - c01) * 64 + fidx * 32 + ky
    with scope("j_rawwait"):
        wait_all(raw_recv, 15, raw_rs)

    def rotate(j):
        lanes = pl.ds(pl.multiple_of(j * 256, 256), 256)
        raw = raw_recv[j].astype(jnp.float32)
        re = jnp.concatenate([raw[:8], raw[16:24]], 1)
        im = jnp.concatenate([raw[8:16], raw[24:]], 1)
        c = tabr[0, 2:3, lanes]
        s = tabr[1, 2:3, lanes]
        xrot[0:8, lanes] = re * c - im * s
        xrot[8:16, lanes] = im * c + re * s

    with scope("k_rotate"):
        loop(0, 16, rotate)

    for group in range(4):
        with scope("l_totwait"):
            if group == 0:
                @pl.when(core == 0)
                def _():
                    wait_all(tot_recv, 4, tot_rs.at[group])

                @pl.when(core == 1)
                def _():
                    wait_all(tot_recv, 3, tot_rs.at[group])
            else:
                wait_all(tot_recv, 4, tot_rs.at[group])
        with scope("m_main"):
            acc = None
            for n in range(4 * group, 4 * group + 4):
                j = sta_at(GROUPS[group][n % 4])
                lanes = pl.ds(pl.multiple_of(j * 256, 256), 256)
                inv = lax.rsqrt(tot_recv[j].astype(jnp.float32) * (1.0 / 256) + epsilon)
                inv = jnp.concatenate([inv[:8], inv[8:]], 1)
                at = slice(n * 256, n * 256 + 256)
                wbuf[0:8, at] = xrot[0:8, lanes] * inv
                wbuf[8:16, at] = xrot[8:16, lanes] * inv
                rows = []
                for trig in range(2):
                    tab = tabc[trig, :, lanes]
                    for row in range(16):
                        rows.append(wbuf[row : row + 1, at] * tab)
                v = jnp.concatenate(rows, 0).astype(jnp.bfloat16)
                term = lax.dot_general(
                    v, tabt[lanes, :], (((1,), (0,)), ((), ())), preferred_element_type=jnp.float32
                )
                acc = term if acc is None else acc + term
            if group == 0:
                accum[...] = acc
            elif group < 3:
                accum[...] += acc
            else:
                acc = acc + accum[...]

    with scope("n_post"):
        mark = jnp.where(iota((128, 128), 1) < 64, -1.0, 1.0)
        cc, cs, sc, ss = acc[:128, :128], acc[:128, 128:], acc[128:, :128], acc[128:, 128:]
        grid = []

        def seg_sum(a):
            a = a * a
            total = a[:8]
            for g in range(1, 8):
                total = total + a[8 * g : 8 * g + 8]
            return total

        for x, y in ((cc - ss, sc + cs), (cc + ss, sc - cs)):
            y = pltpu.roll(y, 64, 1) * mark
            plus, minus = x + y, x - y
            turned = pltpu.roll(plus[64:], 64, 1)
            grid.append(seg_sum(plus[:64] + turned) + pltpu.roll(seg_sum(plus[:64] - turned), 64, 1))
            turned = pltpu.roll(minus[64:], 64, 1)
            grid.append(seg_sum(minus[:64] - turned) + pltpu.roll(seg_sum(minus[:64] + turned), 64, 1))
        grid = jnp.concatenate(grid, 0) * (1.0 / 32768)
        row = iota((8, 128), 0)
        for n in range(8):
            at = slice(128 * n, 128 * n + 128)
            col = jnp.broadcast_to(pick_col[:, at], (8, 128))
            hit = jnp.broadcast_to(pick_row[:, at], (8, 128))
            total = jnp.zeros((8, 128), jnp.float32)
            for k in range(4):
                values = jnp.take_along_axis(grid[8 * k : 8 * k + 8], col, axis=1)
                total = total + jnp.where(row + 8 * k == hit, values, 0.0)
            pow_send[n] = jnp.sum(total, 0, keepdims=True)
    with scope("o_powsend"):
        for d in range(7, 0, -1):
            pow_copy(d).start()
        pow_recv[own] = pow_send[own]

    with scope("p_sendwait"):
        @pl.when(core == 0)
        def _():
            wait_all(part_recv, 8, part_ss)

        @pl.when(core == 1)
        def _():
            wait_all(part_recv, 7, part_ss)
            wait_all(tot_recv, 16, tot_ss.at[0])
            wait_all(tot_recv, 15, tot_ss.at[1])

        wait_all(raw_recv, 15, raw_ss)

    with scope("q_powwait"):
        wait_all(pow_recv, 7, pow_rs)

    with scope("r_end"):
        for b in range(8):
            out_ref[b : b + 1, :] = pow_recv[b]
        wait_all(pow_recv, 7, pow_ss)


def local(spectra, coords, slowness):
    f32, bf16, i32 = jnp.float32, jnp.bfloat16, jnp.int32
    dma = pltpu.SemaphoreType.DMA
    return pl.pallas_call(
        kernel,
        out_shape=jax.ShapeDtypeStruct((8, 128), f32),
        in_specs=[pl.BlockSpec(memory_space=pl.ANY)] * 3,
        out_specs=pl.BlockSpec(memory_space=pltpu.VMEM),
        scratch_shapes=[
            pltpu.VMEM((2, 8, 8, 256), bf16),
            pltpu.VMEM((2, 4096), i32),
            pltpu.VMEM((2, 2048), i32),
            pltpu.VMEM((8, 32, 128), bf16),
            pltpu.VMEM((16, 32, 128), bf16),
            pltpu.VMEM((16, 128), bf16),
            pltpu.VMEM((16, 16, 128), bf16),
            pltpu.VMEM((16, 128), bf16),
            pltpu.VMEM((16, 16, 128), bf16),
            pltpu.VMEM((8, 1, 128), f32),
            pltpu.VMEM((8, 1, 128), f32),
            pltpu.VMEM((2, 8, 4096), f32),
            pltpu.VMEM((4096, 256), bf16),
            pltpu.VMEM((2, 8, 4096), f32),
            pltpu.VMEM((16, 4096), f32),
            pltpu.VMEM((16, 4096), f32),
            pltpu.VMEM((256, 256), f32),
            dma((3,)),
            dma, dma, dma, dma, dma((2,)), dma((4,)), dma, dma,
        ],
        compiler_params=pltpu.CompilerParams(
            collective_id=0, has_side_effects=True, vmem_limit_bytes=56540000
        ),
    )(spectra, coords, slowness)


def solution(mesh):
    in_specs = (P(None, "bins", None, "sta"), P(), P())
    out_specs = P("bins", "sta")
    return jax.shard_map(local, mesh=mesh, in_specs=in_specs, out_specs=out_specs, check_vma=False)
```

```python
import jax
import jax.numpy as jnp
import numpy as np
from jax import lax
from jax.experimental import pallas as pl
from jax.experimental.pallas import tpu as pltpu
from jax.sharding import PartitionSpec as P

MESH = pl.DeviceIdType.MESH
epsilon = 1e-06
scope = jax.named_scope

FAR_Y = (2, 1, 3, 0)
FAR_BINS = sorted(((dx, dl) for dx in range(4) for dl in range(2)), key=lambda o: -min(o[0], 4 - o[0]) - o[1])


def cheb_fit(fn, degree):
    nodes = np.cos(np.pi * (np.arange(4001) + 0.5) / 4001)
    u = (nodes + 1.0) / 2.0
    return np.polynomial.chebyshev.Chebyshev.fit(u, fn(u), degree, domain=[0, 1]).convert(
        kind=np.polynomial.Polynomial
    ).coef


COS = [float(c) for c in cheb_fit(lambda u: np.cos(np.pi * np.sqrt(u)), 7)]
SIN = [float(c) for c in cheb_fit(lambda u: np.pi * np.sinc(np.sqrt(u)), 6)]


def horner(coefs, u):
    acc = jnp.full_like(u, coefs[-1])
    for c in coefs[-2::-1]:
        acc = acc * u + c
    return acc


def cos_sin(index):
    t = lax.shift_right_arithmetic(lax.shift_left(index, 11), 11).astype(jnp.float32) * (1.0 / 1048576)
    u = t * t
    return horner(COS, u), horner(SIN, u) * t


def iota(shape, dim):
    return lax.broadcasted_iota(jnp.int32, shape, dim)


def kernel(
    x_hbm, co_hbm, sl_hbm, out_ref,
    xv, cov, slv, raw_send, raw_recv, part_send, part_recv, tot_send, tot_recv, pow_send, pow_recv,
    tabc, tabt, tabr, xrot, wbuf, accum,
    in_sem, late_sem, part_ss, part_rs, raw_ss, raw_rs, tot_ss, tot_rs, pow_ss, pow_rs,
):
    bi = lax.axis_index("bins")
    sj = lax.axis_index("sta")
    core = lax.rem(bi, 2)
    chip = bi - core
    px = lax.div(bi, 4)
    pl_lo = lax.rem(lax.div(bi, 2), 2)
    pz = lax.div(sj, 4)
    py = lax.rem(sj, 4)
    pair = lax.div(sj, 8)
    own = lax.rem(sj, 8)
    f1 = bi * 8 + own + 1

    early = pz < 2
    late = pz >= 2
    rows = (pz, pz + 1 - 2 * lax.rem(pz, 2), 3 - pz, lax.rem(pz + 2, 4))

    def sta_at(n, dy):
        return rows[n] * 4 + lax.rem(py + dy, 4)

    def chip_at(o):
        return lax.rem(px + o[0], 4) * 4 + lax.rem(pl_lo + o[1], 2) * 2

    loads = [
        pltpu.make_async_copy(src, dst, in_sem.at[n])
        for n, (src, dst) in enumerate(((x_hbm, xv), (co_hbm, cov), (sl_hbm, slv)))
    ]
    for load in loads:
        load.start()

    barrier = pltpu.get_barrier_semaphore()

    def greet(b, s):
        pl.semaphore_signal(barrier, inc=1, device_id=(b, s), device_id_type=MESH)

    def loop(lo, hi, body):
        lax.fori_loop(lo, hi, lambda d, c: (body(d), c)[1], 0)

    def greet_rows(b, first, last):
        loop(first * 4, last * 4, lambda q: greet(b, q))

    def greet_peers(first, last):
        @pl.when((pz >= first) & (pz < last))
        def _():
            loop(1, 4 * (last - first), lambda d: greet(bi, first * 4 + lax.rem(sj - first * 4 + d, 4 * (last - first))))

        @pl.when((pz < first) | (pz >= last))
        def _():
            greet_rows(bi, first, last)

    with scope("a_greet"):
        @pl.when(core == 1)
        def _():
            for o in FAR_BINS:
                greet(chip_at(o), sj)
                if o != (0, 0):
                    greet(chip_at(o) + 1, sj)

            @pl.when(early)
            def _():
                greet_rows(chip, 2, 4)

        @pl.when(core == 0)
        def _():
            greet_rows(chip + 1, 2, 4)

            @pl.when(early)
            def _():
                greet_rows(chip + 1, 0, 2)

        greet_peers(2, 4)

        @pl.when(early)
        def _():
            greet_peers(0, 2)

    with scope("b_xwait"):
        loads[0].wait()

    with scope("c_sumsq"):
        sq = jnp.zeros((8, 256), jnp.float32)
        for b in range(8):
            re = xv[0, b].astype(jnp.float32)
            im = xv[1, b].astype(jnp.float32)
            sq = sq + (re * re + im * im)
            raw_send[b] = jnp.concatenate(
                [re[:, :128], im[:, :128], re[:, 128:], im[:, 128:]], 0
            ).astype(jnp.bfloat16)
        part = jnp.concatenate([sq[:, :128], sq[:, 128:]], 0).astype(jnp.bfloat16)
        part_send[...] = part

    with scope("d_barrier"):
        for cond, count in (
            (early & (core == 1), 22), (late & (core == 1), 38), (early & (core == 0), 15), (late & (core == 0), 31)
        ):
            @pl.when(cond)
            def _(count=count):
                pl.semaphore_wait(barrier, count)

    def part_copy(n):
        return pltpu.make_async_remote_copy(
            src_ref=part_send, dst_ref=part_recv.at[bi],
            send_sem=part_ss, recv_sem=part_rs,
            device_id=(chip_at(FAR_BINS[n]) + 1, sj), device_id_type=MESH,
        )

    def raw_copy(n, dy):
        q = sta_at(n, dy)
        return pltpu.make_async_remote_copy(
            src_ref=raw_send.at[lax.rem(q, 8)], dst_ref=raw_recv.at[sj],
            send_sem=raw_ss, recv_sem=raw_rs.at[n // 2],
            device_id=(bi, q), device_id_type=MESH,
        )

    def tot_copy(n, dy, c):
        return pltpu.make_async_remote_copy(
            src_ref=tot_send, dst_ref=tot_recv.at[sj],
            send_sem=tot_ss.at[c], recv_sem=tot_rs.at[n],
            device_id=(chip + c, sta_at(n, dy)), device_id_type=MESH,
        )

    def send_raw(n):
        for dy in FAR_Y:
            if (n, dy) != (0, 0):
                raw_copy(n, dy).start()

    def send_tot(n):
        for dy in FAR_Y:
            tot_copy(n, dy, 0).start()
            if (n, dy) != (0, 0):
                tot_copy(n, dy, 1).start()

    def pow_copy(d):
        m = lax.rem(own + d, 8)
        return pltpu.make_async_remote_copy(
            src_ref=pow_send.at[m], dst_ref=pow_recv.at[own],
            send_sem=pow_ss, recv_sem=pow_rs,
            device_id=(bi, pair * 8 + m), device_id_type=MESH,
        )

    def wait_all(buf, count, sem):
        blocks = buf.at[pl.ds(0, count)]
        pltpu.make_async_copy(blocks, blocks, sem).wait()

    with scope("e_send1"):
        for n in range(7):
            part_copy(n).start()

        @pl.when(core == 0)
        def _():
            part_copy(7).start()

        @pl.when(core == 1)
        def _():
            part_recv[bi] = part

        @pl.when(late)
        def _():
            def announce(b):
                loop(0, 8, lambda q: pl.semaphore_signal(late_sem, inc=1, device_id=(b, q), device_id_type=MESH))

            announce(bi)

            @pl.when(core == 0)
            def _():
                announce(chip + 1)

            send_raw(3)
            send_raw(2)

        send_raw(1)
        send_raw(0)
        raw_recv[sj] = raw_send[own]

    loads[1].wait()
    loads[2].wait()
    row8 = iota((8, 256), 0)
    odd32 = iota((32, 256), 0) * 2 + 1
    coarse = row8 * 8 + 4
    fine = jnp.where(row8 == 0, 1, 3)

    def tables(j):
        lanes = pl.ds(pl.multiple_of(j * 256, 256), 256)
        cx = cov[0:1, lanes] * f1
        cy = cov[1:2, lanes] * f1
        c, s = cos_sin(coarse * cx)
        tabc[0, :, lanes] = c
        tabc[1, :, lanes] = s
        c, s = cos_sin(jnp.where(row8 < 2, fine * cx, jnp.broadcast_to(cx + cy, (8, 256))))
        tabr[0, :, lanes] = c
        tabr[1, :, lanes] = s
        cyt, syt = cos_sin(odd32 * cy)
        cols = []
        for trig in range(2):
            for tab in (cyt, syt):
                for f in range(2):
                    cols.append(tabr[trig, f : f + 1, lanes] * tab)
        tabt[lanes, :] = jnp.concatenate(cols, 0).astype(jnp.bfloat16).T

    with scope("f_tables"):
        loop(0, 16, tables)

    @pl.when(core == 1)
    def _():
        with scope("g_partwait"):
            wait_all(part_recv, 15, part_rs)
        with scope("h_total"):
            total = part_recv[0].astype(jnp.float32)
            for p in range(1, 16):
                total = total + part_recv[p].astype(jnp.float32)
            total = total.astype(jnp.bfloat16)
            tot_send[...] = total

            @pl.when(late)
            def _():
                send_tot(3)
                send_tot(2)

            send_tot(1)
            send_tot(0)
            tot_recv[sj] = total

    with scope("i_pick"):
        beams = pl.ds(pl.multiple_of(pair * 1024, 1024), 1024)
        sx = slv[0:1, beams]
        sy = slv[1:2, beams]
        u = sx + 32
        m = lax.shift_right_arithmetic(u, 2)
        f = u & 3
        cpos = m >= 8
        fpos = f >= 2
        ypos = sy >= 0
        cidx = jnp.where(cpos, m - 8, 7 - m)
        fidx = jnp.where(fpos, f - 2, 1 - f)
        ky = jnp.where(ypos, sy, -1 - sy)
        c01 = jnp.where(cpos, 1, 0)
        rel = jnp.where(c01 == jnp.where(fpos, 1, 0), 0, 1)
        diff = jnp.where(c01 == jnp.where(ypos, 1, 0), 0, 1)
        pick_row = (rel * 2 + diff) * 8 + cidx
        pick_col = (1 - c01) * 64 + fidx * 32 + ky
    with scope("i_late"):
        @pl.when(early & (core == 1))
        def _():
            pl.semaphore_wait(late_sem, 16)
            send_tot(2)
            send_tot(3)

        @pl.when(early & (core == 0))
        def _():
            pl.semaphore_wait(late_sem, 8)

        @pl.when(early)
        def _():
            send_raw(2)
            send_raw(3)

    def rotate(n):
        def block(y):
            j = rows[n] * 4 + y
            lanes = pl.ds(pl.multiple_of(j * 256, 256), 256)
            raw = raw_recv[j].astype(jnp.float32)
            re = jnp.concatenate([raw[:8], raw[16:24]], 1)
            im = jnp.concatenate([raw[8:16], raw[24:]], 1)
            c = tabr[0, 2:3, lanes]
            s = tabr[1, 2:3, lanes]
            xrot[0:8, lanes] = re * c - im * s
            xrot[8:16, lanes] = im * c + re * s

        loop(0, 4, block)

    for n in range(4):
        if n % 2 == 0:
            with scope("j_rawwait"):
                wait_all(raw_recv, 7 + n // 2, raw_rs.at[n // 2])
            with scope("k_rotate"):
                rotate(n)
                rotate(n + 1)
        with scope("l_totwait%d" % n):
            if n == 0:
                @pl.when(core == 0)
                def _():
                    wait_all(tot_recv, 4, tot_rs.at[0])

                @pl.when(core == 1)
                def _():
                    wait_all(tot_recv, 3, tot_rs.at[0])
            else:
                wait_all(tot_recv, 4, tot_rs.at[n])
        with scope("m_main"):
            lanes = pl.ds(pl.multiple_of(rows[n] * 1024, 1024), 1024)
            at = slice(n * 1024, n * 1024 + 1024)
            parts = []
            for y in range(4):
                total = tot_recv[rows[n] * 4 + y].astype(jnp.float32)
                parts += [total[:8], total[8:]]
            inv = lax.rsqrt(jnp.concatenate(parts, 1) * (1.0 / 256) + epsilon)
            wbuf[0:8, at] = xrot[0:8, lanes] * inv
            wbuf[8:16, at] = xrot[8:16, lanes] * inv
            v = []
            for trig in range(2):
                tab = tabc[trig, :, lanes]
                for row in range(16):
                    v.append(wbuf[row : row + 1, at] * tab)
            acc = jnp.dot(
                jnp.concatenate(v, 0).astype(jnp.bfloat16), tabt[lanes, :], preferred_element_type=jnp.float32
            )
            if n == 0:
                accum[...] = acc
            elif n < 3:
                accum[...] += acc
            else:
                acc = acc + accum[...]

    with scope("n_post"):
        mark = jnp.where(iota((128, 128), 1) < 64, -1.0, 1.0)
        cc, cs, sc, ss = acc[:128, :128], acc[:128, 128:], acc[128:, :128], acc[128:, 128:]
        grid = []

        def seg_sum(a):
            a = a * a
            total = a[:8]
            for g in range(1, 8):
                total = total + a[8 * g : 8 * g + 8]
            return total

        for x, y in ((cc - ss, sc + cs), (cc + ss, sc - cs)):
            y = pltpu.roll(y, 64, 1) * mark
            plus, minus = x + y, x - y
            turned = pltpu.roll(plus[64:], 64, 1)
            grid.append(seg_sum(plus[:64] + turned) + pltpu.roll(seg_sum(plus[:64] - turned), 64, 1))
            turned = pltpu.roll(minus[64:], 64, 1)
            grid.append(seg_sum(minus[:64] - turned) + pltpu.roll(seg_sum(minus[:64] + turned), 64, 1))
        grid = jnp.concatenate(grid, 0) * (1.0 / 32768)
        row = iota((8, 128), 0)
        for n in range(8):
            at = slice(128 * n, 128 * n + 128)
            col = jnp.broadcast_to(pick_col[:, at], (8, 128))
            hit = jnp.broadcast_to(pick_row[:, at], (8, 128))
            total = jnp.zeros((8, 128), jnp.float32)
            for k in range(4):
                values = jnp.take_along_axis(grid[8 * k : 8 * k + 8], col, axis=1)
                total = total + jnp.where(row + 8 * k == hit, values, 0.0)
            pow_send[n] = jnp.sum(total, 0, keepdims=True)
    with scope("o_powsend"):
        for d in range(7, 0, -1):
            pow_copy(d).start()
        pow_recv[own] = pow_send[own]

    with scope("p_sendwait"):
        @pl.when(core == 0)
        def _():
            wait_all(part_recv, 8, part_ss)

        @pl.when(core == 1)
        def _():
            wait_all(part_recv, 7, part_ss)
            wait_all(tot_recv, 16, tot_ss.at[0])
            wait_all(tot_recv, 15, tot_ss.at[1])

        wait_all(raw_recv, 15, raw_ss)

    with scope("q_powwait"):
        wait_all(pow_recv, 7, pow_rs)

    with scope("r_end"):
        for b in range(8):
            out_ref[b : b + 1, :] = pow_recv[b]
        wait_all(pow_recv, 7, pow_ss)


def local(spectra, coords, slowness):
    f32, bf16, i32 = jnp.float32, jnp.bfloat16, jnp.int32
    dma = pltpu.SemaphoreType.DMA
    return pl.pallas_call(
        kernel,
        out_shape=jax.ShapeDtypeStruct((8, 128), f32),
        in_specs=[pl.BlockSpec(memory_space=pl.ANY)] * 3,
        out_specs=pl.BlockSpec(memory_space=pltpu.VMEM),
        scratch_shapes=[
            pltpu.VMEM((2, 8, 8, 256), bf16),
            pltpu.VMEM((2, 4096), i32),
            pltpu.VMEM((2, 2048), i32),
            pltpu.VMEM((8, 32, 128), bf16),
            pltpu.VMEM((16, 32, 128), bf16),
            pltpu.VMEM((16, 128), bf16),
            pltpu.VMEM((16, 16, 128), bf16),
            pltpu.VMEM((16, 128), bf16),
            pltpu.VMEM((16, 16, 128), bf16),
            pltpu.VMEM((8, 1, 128), f32),
            pltpu.VMEM((8, 1, 128), f32),
            pltpu.VMEM((2, 8, 4096), f32),
            pltpu.VMEM((4096, 256), bf16),
            pltpu.VMEM((2, 8, 4096), f32),
            pltpu.VMEM((16, 4096), f32),
            pltpu.VMEM((16, 4096), f32),
            pltpu.VMEM((256, 256), f32),
            dma((3,)),
            pltpu.SemaphoreType.REGULAR,
            dma, dma, dma, dma((2,)), dma((2,)), dma((4,)), dma, dma,
        ],
        compiler_params=pltpu.CompilerParams(
            collective_id=0, has_side_effects=True, vmem_limit_bytes=56540000
        ),
    )(spectra, coords, slowness)


def solution(mesh):
    in_specs = (P(None, "bins", None, "sta"), P(), P())
    out_specs = P("bins", "sta")
    return jax.shard_map(local, mesh=mesh, in_specs=in_specs, out_specs=out_specs, check_vma=False)
```

```python
import jax
import jax.numpy as jnp
import numpy as np
from jax import lax
from jax.experimental import pallas as pl
from jax.experimental.pallas import tpu as pltpu
from jax.sharding import PartitionSpec as P

MESH = pl.DeviceIdType.MESH
epsilon = 1e-06
scope = jax.named_scope

FAR_Y = (2, 1, 3, 0)
FAR_BINS = sorted(((dx, dl) for dx in range(4) for dl in range(2)), key=lambda o: -min(o[0], 4 - o[0]) - o[1])


def cheb_fit(fn, degree):
    nodes = np.cos(np.pi * (np.arange(4001) + 0.5) / 4001)
    u = (nodes + 1.0) / 2.0
    return np.polynomial.chebyshev.Chebyshev.fit(u, fn(u), degree, domain=[0, 1]).convert(
        kind=np.polynomial.Polynomial
    ).coef


COS = [float(c) for c in cheb_fit(lambda u: np.cos(np.pi * np.sqrt(u)), 7)]
SIN = [float(c) for c in cheb_fit(lambda u: np.pi * np.sinc(np.sqrt(u)), 6)]


def horner(coefs, u):
    acc = jnp.full_like(u, coefs[-1])
    for c in coefs[-2::-1]:
        acc = acc * u + c
    return acc


def cos_sin(index):
    t = lax.shift_right_arithmetic(lax.shift_left(index, 11), 11).astype(jnp.float32) * (1.0 / 1048576)
    u = t * t
    return horner(COS, u), horner(SIN, u) * t


def iota(shape, dim):
    return lax.broadcasted_iota(jnp.int32, shape, dim)


def kernel(
    x_hbm, co_hbm, sl_hbm, out_ref,
    xv, cov, slv, raw_send, raw_recv, side_send, side_recv, part_send, part_recv, tot_send, tot_recv, pow_send, pow_recv,
    tabc, tabt, tabr, xrot, wbuf, accum,
    in_sem, late_sem, go_sem, side_ss, side_rs, part_ss, part_rs, raw_ss, raw_rs, tot_ss, tot_rs, pow_ss, pow_rs,
):
    bi = lax.axis_index("bins")
    sj = lax.axis_index("sta")
    core = lax.rem(bi, 2)
    chip = bi - core
    px = lax.div(bi, 4)
    pl_lo = lax.rem(lax.div(bi, 2), 2)
    pz = lax.div(sj, 4)
    py = lax.rem(sj, 4)
    pair = lax.div(sj, 8)
    own = lax.rem(sj, 8)
    f1 = bi * 8 + own + 1

    early = pz < 2
    late = pz >= 2
    rows = (pz, pz + 1 - 2 * lax.rem(pz, 2), 3 - pz, lax.rem(pz + 2, 4))

    def sta_at(n, dy):
        return rows[n] * 4 + lax.rem(py + dy, 4)

    def chip_at(o):
        return lax.rem(px + o[0], 4) * 4 + lax.rem(pl_lo + o[1], 2) * 2

    loads = [
        pltpu.make_async_copy(src, dst, in_sem.at[n])
        for n, (src, dst) in enumerate(((x_hbm, xv), (co_hbm, cov), (sl_hbm, slv)))
    ]
    for load in loads:
        load.start()

    barrier = pltpu.get_barrier_semaphore()

    def greet(b, s):
        pl.semaphore_signal(barrier, inc=1, device_id=(b, s), device_id_type=MESH)

    def loop(lo, hi, body):
        lax.fori_loop(lo, hi, lambda d, c: (body(d), c)[1], 0)

    with scope("a_greet"):
        @pl.when(core == 1)
        def _():
            greet(chip, sj)
            for o in FAR_BINS[:7]:
                greet(chip_at(o) + 1, sj)

            @pl.when(early)
            def _():
                loop(1, 16, lambda d: greet(bi, lax.rem(sj + d, 16)))

            @pl.when(late)
            def _():
                loop(1, 8, lambda d: greet(bi, 8 + lax.rem(sj + d, 8)))

        @pl.when(early & (core == 0))
        def _():
            loop(1, 16, lambda d: greet(chip + 1, lax.rem(sj + d, 16)))

    with scope("b_xwait"):
        loads[0].wait()

    with scope("c_sumsq"):
        sq = jnp.zeros((8, 256), jnp.float32)
        for b in range(8):
            re = xv[0, b].astype(jnp.float32)
            im = xv[1, b].astype(jnp.float32)
            sq = sq + (re * re + im * im)
            raw_send[b] = jnp.concatenate(
                [re[:, :128], im[:, :128], re[:, 128:], im[:, 128:]], 0
            ).astype(jnp.bfloat16)
        side = jnp.concatenate([sq[:, :128], sq[:, 128:]], 0)
        side_send[...] = side

    side_copy = pltpu.make_async_remote_copy(
        src_ref=side_send, dst_ref=side_recv, send_sem=side_ss, recv_sem=side_rs,
        device_id=(chip + 1, sj), device_id_type=MESH,
    )

    def go(n):
        pl.semaphore_signal(go_sem.at[n], inc=1, device_id=(chip, sj), device_id_type=MESH)

    def part_copy(n):
        return pltpu.make_async_remote_copy(
            src_ref=part_send, dst_ref=part_recv.at[lax.div(bi, 2)],
            send_sem=part_ss, recv_sem=part_rs,
            device_id=(chip_at(FAR_BINS[n]) + 1, sj), device_id_type=MESH,
        )

    def raw_copy(n, dy):
        q = sta_at(n, dy)
        return pltpu.make_async_remote_copy(
            src_ref=raw_send.at[lax.rem(q, 8)], dst_ref=raw_recv.at[sj],
            send_sem=raw_ss, recv_sem=raw_rs.at[n // 2],
            device_id=(bi, q), device_id_type=MESH,
        )

    def tot_copy(n, dy, c):
        return pltpu.make_async_remote_copy(
            src_ref=tot_send, dst_ref=tot_recv.at[sj],
            send_sem=tot_ss.at[c], recv_sem=tot_rs.at[n],
            device_id=(chip + c, sta_at(n, dy)), device_id_type=MESH,
        )

    def send_raw(n):
        for dy in FAR_Y:
            if (n, dy) != (0, 0):
                raw_copy(n, dy).start()

    def send_tot(n):
        for dy in FAR_Y:
            tot_copy(n, dy, 0).start()
            if (n, dy) != (0, 0):
                tot_copy(n, dy, 1).start()

    def pow_copy(d):
        m = lax.rem(own + d, 8)
        return pltpu.make_async_remote_copy(
            src_ref=pow_send.at[m], dst_ref=pow_recv.at[own],
            send_sem=pow_ss, recv_sem=pow_rs,
            device_id=(bi, pair * 8 + m), device_id_type=MESH,
        )

    def wait_all(buf, count, sem):
        blocks = buf.at[pl.ds(0, count)]
        pltpu.make_async_copy(blocks, blocks, sem).wait()

    with scope("d_barrier"):
        @pl.when(early & (core == 1))
        def _():
            pl.semaphore_wait(barrier, 21)

        @pl.when(late & (core == 1))
        def _():
            pl.semaphore_wait(barrier, 30)

        @pl.when(core == 0)
        def _():
            pl.semaphore_wait(barrier, 1)
            side_copy.start()

    with scope("e_side"):
        @pl.when(core == 1)
        def _():
            side_copy.wait_recv()
            part = (side + side_recv[...]).astype(jnp.bfloat16)
            part_send[...] = part
            for n in range(7):
                part_copy(n).start()
            go(0)
            part_recv[lax.div(bi, 2)] = part

            def announce(first, last):
                def one(q):
                    @pl.when(q != sj)
                    def _():
                        pl.semaphore_signal(late_sem, inc=1, device_id=(bi, q), device_id_type=MESH)

                loop(first, last, one)

            @pl.when(late)
            def _():
                announce(0, 16)

        @pl.when(core == 0)
        def _():
            pl.semaphore_wait(go_sem.at[0], 1)

    with scope("e_send1"):
        @pl.when(late)
        def _():
            send_raw(3)
            send_raw(2)

        @pl.when(early)
        def _():
            send_raw(1)
            send_raw(0)

        raw_recv[sj] = raw_send[own]

    loads[1].wait()
    loads[2].wait()
    row8 = iota((8, 256), 0)
    odd32 = iota((32, 256), 0) * 2 + 1
    coarse = row8 * 8 + 4
    fine = jnp.where(row8 == 0, 1, 3)

    def tables(j):
        lanes = pl.ds(pl.multiple_of(j * 256, 256), 256)
        cx = cov[0:1, lanes] * f1
        cy = cov[1:2, lanes] * f1
        c, s = cos_sin(coarse * cx)
        tabc[0, :, lanes] = c
        tabc[1, :, lanes] = s
        c, s = cos_sin(jnp.where(row8 < 2, fine * cx, jnp.broadcast_to(cx + cy, (8, 256))))
        tabr[0, :, lanes] = c
        tabr[1, :, lanes] = s
        cyt, syt = cos_sin(odd32 * cy)
        cols = []
        for trig in range(2):
            for tab in (cyt, syt):
                for f in range(2):
                    cols.append(tabr[trig, f : f + 1, lanes] * tab)
        tabt[lanes, :] = jnp.concatenate(cols, 0).astype(jnp.bfloat16).T

    with scope("f_tables"):
        loop(0, 16, tables)

    @pl.when(core == 1)
    def _():
        with scope("g_partwait"):
            wait_all(part_recv, 7, part_rs)
        with scope("h_total"):
            total = part_recv[0].astype(jnp.float32)
            for p in range(1, 8):
                total = total + part_recv[p].astype(jnp.float32)
            total = total.astype(jnp.bfloat16)
            tot_send[...] = total

            @pl.when(late)
            def _():
                send_tot(3)
                send_tot(2)

            @pl.when(early)
            def _():
                send_tot(1)
                send_tot(0)

            tot_recv[sj] = total

    with scope("i_pick"):
        beams = pl.ds(pl.multiple_of(pair * 1024, 1024), 1024)
        sx = slv[0:1, beams]
        sy = slv[1:2, beams]
        u = sx + 32
        m = lax.shift_right_arithmetic(u, 2)
        f = u & 3
        cpos = m >= 8
        fpos = f >= 2
        ypos = sy >= 0
        cidx = jnp.where(cpos, m - 8, 7 - m)
        fidx = jnp.where(fpos, f - 2, 1 - f)
        ky = jnp.where(ypos, sy, -1 - sy)
        c01 = jnp.where(cpos, 1, 0)
        rel = jnp.where(c01 == jnp.where(fpos, 1, 0), 0, 1)
        diff = jnp.where(c01 == jnp.where(ypos, 1, 0), 0, 1)
        pick_row = (rel * 2 + diff) * 8 + cidx
        pick_col = (1 - c01) * 64 + fidx * 32 + ky
    with scope("i_late"):
        @pl.when(early & (core == 1))
        def _():
            pl.semaphore_wait(late_sem, 8)
            go(1)
            send_tot(2)
            send_tot(3)

        @pl.when(late & (core == 1))
        def _():
            pl.semaphore_wait(late_sem, 7)
            go(1)
            send_tot(1)
            send_tot(0)

        @pl.when(core == 0)
        def _():
            pl.semaphore_wait(go_sem.at[1], 1)

        @pl.when(early)
        def _():
            send_raw(2)
            send_raw(3)

        @pl.when(late)
        def _():
            send_raw(1)
            send_raw(0)

    def rotate(n):
        def block(y):
            j = rows[n] * 4 + y
            lanes = pl.ds(pl.multiple_of(j * 256, 256), 256)
            raw = raw_recv[j].astype(jnp.float32)
            re = jnp.concatenate([raw[:8], raw[16:24]], 1)
            im = jnp.concatenate([raw[8:16], raw[24:]], 1)
            c = tabr[0, 2:3, lanes]
            s = tabr[1, 2:3, lanes]
            xrot[0:8, lanes] = re * c - im * s
            xrot[8:16, lanes] = im * c + re * s

        loop(0, 4, block)

    for n in range(4):
        if n % 2 == 0:
            with scope("j_rawwait"):
                wait_all(raw_recv, 7 + n // 2, raw_rs.at[n // 2])
            with scope("k_rotate"):
                rotate(n)
                rotate(n + 1)
        with scope("l_totwait%d" % n):
            if n == 0:
                @pl.when(core == 0)
                def _():
                    wait_all(tot_recv, 4, tot_rs.at[0])

                @pl.when(core == 1)
                def _():
                    wait_all(tot_recv, 3, tot_rs.at[0])
            else:
                wait_all(tot_recv, 4, tot_rs.at[n])
        with scope("m_main"):
            lanes = pl.ds(pl.multiple_of(rows[n] * 1024, 1024), 1024)
            at = slice(n * 1024, n * 1024 + 1024)
            parts = []
            for y in range(4):
                total = tot_recv[rows[n] * 4 + y].astype(jnp.float32)
                parts += [total[:8], total[8:]]
            inv = lax.rsqrt(jnp.concatenate(parts, 1) * (1.0 / 256) + epsilon)
            wbuf[0:8, at] = xrot[0:8, lanes] * inv
            wbuf[8:16, at] = xrot[8:16, lanes] * inv
            v = []
            for trig in range(2):
                tab = tabc[trig, :, lanes]
                for row in range(16):
                    v.append(wbuf[row : row + 1, at] * tab)
            acc = jnp.dot(
                jnp.concatenate(v, 0).astype(jnp.bfloat16), tabt[lanes, :], preferred_element_type=jnp.float32
            )
            if n == 0:
                accum[...] = acc
            elif n < 3:
                accum[...] += acc
            else:
                acc = acc + accum[...]

    with scope("n_post"):
        mark = jnp.where(iota((128, 128), 1) < 64, -1.0, 1.0)
        cc, cs, sc, ss = acc[:128, :128], acc[:128, 128:], acc[128:, :128], acc[128:, 128:]
        grid = []

        def seg_sum(a):
            a = a * a
            total = a[:8]
            for g in range(1, 8):
                total = total + a[8 * g : 8 * g + 8]
            return total

        for x, y in ((cc - ss, sc + cs), (cc + ss, sc - cs)):
            y = pltpu.roll(y, 64, 1) * mark
            plus, minus = x + y, x - y
            turned = pltpu.roll(plus[64:], 64, 1)
            grid.append(seg_sum(plus[:64] + turned) + pltpu.roll(seg_sum(plus[:64] - turned), 64, 1))
            turned = pltpu.roll(minus[64:], 64, 1)
            grid.append(seg_sum(minus[:64] - turned) + pltpu.roll(seg_sum(minus[:64] + turned), 64, 1))
        grid = jnp.concatenate(grid, 0) * (1.0 / 32768)
        row = iota((8, 128), 0)
        for n in range(8):
            at = slice(128 * n, 128 * n + 128)
            col = jnp.broadcast_to(pick_col[:, at], (8, 128))
            hit = jnp.broadcast_to(pick_row[:, at], (8, 128))
            total = jnp.zeros((8, 128), jnp.float32)
            for k in range(4):
                values = jnp.take_along_axis(grid[8 * k : 8 * k + 8], col, axis=1)
                total = total + jnp.where(row + 8 * k == hit, values, 0.0)
            pow_send[n] = jnp.sum(total, 0, keepdims=True)
    with scope("o_powsend"):
        for d in range(7, 0, -1):
            pow_copy(d).start()
        pow_recv[own] = pow_send[own]

    with scope("p_sendwait"):
        @pl.when(core == 0)
        def _():
            side_copy.wait_send()

        @pl.when(core == 1)
        def _():
            wait_all(part_recv, 7, part_ss)
            wait_all(tot_recv, 16, tot_ss.at[0])
            wait_all(tot_recv, 15, tot_ss.at[1])

        wait_all(raw_recv, 15, raw_ss)

    with scope("q_powwait"):
        wait_all(pow_recv, 7, pow_rs)

    with scope("r_end"):
        for b in range(8):
            out_ref[b : b + 1, :] = pow_recv[b]
        wait_all(pow_recv, 7, pow_ss)


def local(spectra, coords, slowness):
    f32, bf16, i32 = jnp.float32, jnp.bfloat16, jnp.int32
    dma = pltpu.SemaphoreType.DMA
    return pl.pallas_call(
        kernel,
        out_shape=jax.ShapeDtypeStruct((8, 128), f32),
        in_specs=[pl.BlockSpec(memory_space=pl.ANY)] * 3,
        out_specs=pl.BlockSpec(memory_space=pltpu.VMEM),
        scratch_shapes=[
            pltpu.VMEM((2, 8, 8, 256), bf16),
            pltpu.VMEM((2, 4096), i32),
            pltpu.VMEM((2, 2048), i32),
            pltpu.VMEM((8, 32, 128), bf16),
            pltpu.VMEM((16, 32, 128), bf16),
            pltpu.VMEM((16, 128), f32),
            pltpu.VMEM((16, 128), f32),
            pltpu.VMEM((16, 128), bf16),
            pltpu.VMEM((8, 16, 128), bf16),
            pltpu.VMEM((16, 128), bf16),
            pltpu.VMEM((16, 16, 128), bf16),
            pltpu.VMEM((8, 1, 128), f32),
            pltpu.VMEM((8, 1, 128), f32),
            pltpu.VMEM((2, 8, 4096), f32),
            pltpu.VMEM((4096, 256), bf16),
            pltpu.VMEM((2, 8, 4096), f32),
            pltpu.VMEM((16, 4096), f32),
            pltpu.VMEM((16, 4096), f32),
            pltpu.VMEM((256, 256), f32),
            dma((3,)),
            pltpu.SemaphoreType.REGULAR,
            pltpu.SemaphoreType.REGULAR((2,)),
            dma, dma,
            dma, dma, dma, dma((2,)), dma((2,)), dma((4,)), dma, dma,
        ],
        compiler_params=pltpu.CompilerParams(
            collective_id=0, has_side_effects=True, vmem_limit_bytes=56540000
        ),
    )(spectra, coords, slowness)


def solution(mesh):
    in_specs = (P(None, "bins", None, "sta"), P(), P())
    out_specs = P("bins", "sta")
    return jax.shard_map(local, mesh=mesh, in_specs=in_specs, out_specs=out_specs, check_vma=False)
```

```python
import jax
import jax.numpy as jnp
import numpy as np
from jax import lax
from jax.experimental import pallas as pl
from jax.experimental.pallas import tpu as pltpu
from jax.sharding import PartitionSpec as P

MESH = pl.DeviceIdType.MESH
epsilon = 1e-06
scope = jax.named_scope

FAR_Y = (2, 1, 3, 0)
FAR_BINS = sorted(((dx, dl) for dx in range(4) for dl in range(2)), key=lambda o: -min(o[0], 4 - o[0]) - o[1])


def cheb_fit(fn, degree):
    nodes = np.cos(np.pi * (np.arange(4001) + 0.5) / 4001)
    u = (nodes + 1.0) / 2.0
    return np.polynomial.chebyshev.Chebyshev.fit(u, fn(u), degree, domain=[0, 1]).convert(
        kind=np.polynomial.Polynomial
    ).coef


COS = [float(c) for c in cheb_fit(lambda u: np.cos(np.pi * np.sqrt(u)), 7)]
SIN = [float(c) for c in cheb_fit(lambda u: np.pi * np.sinc(np.sqrt(u)), 6)]


def horner(coefs, u):
    acc = jnp.full_like(u, coefs[-1])
    for c in coefs[-2::-1]:
        acc = acc * u + c
    return acc


def cos_sin(index):
    t = lax.shift_right_arithmetic(lax.shift_left(index, 11), 11).astype(jnp.float32) * (1.0 / 1048576)
    u = t * t
    return horner(COS, u), horner(SIN, u) * t


def iota(shape, dim):
    return lax.broadcasted_iota(jnp.int32, shape, dim)


def kernel(
    x_hbm, co_hbm, sl_hbm, out_ref,
    xv, cov, slv, raw_send, raw_recv, side_send, side_recv, part_send, part_recv, tot_send, tot_recv, pow_send, pow_recv,
    tabc, tabt, tabr, xrot, wbuf, accum,
    in_sem, late_sem, go_sem, side_ss, side_rs, part_ss, part_rs, raw_ss, raw_rs, tot_ss, tot_rs, forward_ss, pow_ss, pow_rs,
):
    bi = lax.axis_index("bins")
    sj = lax.axis_index("sta")
    core = lax.rem(bi, 2)
    chip = bi - core
    px = lax.div(bi, 4)
    pl_lo = lax.rem(lax.div(bi, 2), 2)
    pz = lax.div(sj, 4)
    py = lax.rem(sj, 4)
    pair = lax.div(sj, 8)
    own = lax.rem(sj, 8)
    f1 = bi * 8 + own + 1

    early = pz < 2
    late = pz >= 2
    rows = (pz, pz + 1 - 2 * lax.rem(pz, 2), 3 - pz, lax.rem(pz + 2, 4))

    def sta_at(n, dy):
        return rows[n] * 4 + lax.rem(py + dy, 4)

    def chip_at(o):
        return lax.rem(px + o[0], 4) * 4 + lax.rem(pl_lo + o[1], 2) * 2

    loads = [
        pltpu.make_async_copy(src, dst, in_sem.at[n])
        for n, (src, dst) in enumerate(((x_hbm, xv), (co_hbm, cov), (sl_hbm, slv)))
    ]
    for load in loads:
        load.start()

    barrier = pltpu.get_barrier_semaphore()

    def greet(b, s):
        pl.semaphore_signal(barrier, inc=1, device_id=(b, s), device_id_type=MESH)

    def loop(lo, hi, body):
        lax.fori_loop(lo, hi, lambda d, c: (body(d), c)[1], 0)

    with scope("a_greet"):
        @pl.when(core == 1)
        def _():
            greet(chip, sj)
            for o in FAR_BINS[:7]:
                greet(chip_at(o) + 1, sj)

            @pl.when(early)
            def _():
                loop(1, 16, lambda d: greet(bi, lax.rem(sj + d, 16)))

            @pl.when(late)
            def _():
                loop(1, 8, lambda d: greet(bi, 8 + lax.rem(sj + d, 8)))

        @pl.when(early & (core == 0))
        def _():
            loop(1, 16, lambda d: greet(chip + 1, lax.rem(sj + d, 16)))

    with scope("b_xwait"):
        loads[0].wait()

    with scope("c_sumsq"):
        sq = jnp.zeros((8, 256), jnp.float32)
        for b in range(8):
            re = xv[0, b].astype(jnp.float32)
            im = xv[1, b].astype(jnp.float32)
            sq = sq + (re * re + im * im)
            raw_send[b] = jnp.concatenate(
                [re[:, :128], im[:, :128], re[:, 128:], im[:, 128:]], 0
            ).astype(jnp.bfloat16)
        side = jnp.concatenate([sq[:, :128], sq[:, 128:]], 0)
        side_send[...] = side

    side_copy = pltpu.make_async_remote_copy(
        src_ref=side_send, dst_ref=side_recv, send_sem=side_ss, recv_sem=side_rs,
        device_id=(chip + 1, sj), device_id_type=MESH,
    )

    def go(n):
        pl.semaphore_signal(go_sem.at[n], inc=1, device_id=(chip, sj), device_id_type=MESH)

    def part_copy(n):
        return pltpu.make_async_remote_copy(
            src_ref=part_send, dst_ref=part_recv.at[lax.div(bi, 2)],
            send_sem=part_ss, recv_sem=part_rs,
            device_id=(chip_at(FAR_BINS[n]) + 1, sj), device_id_type=MESH,
        )

    def raw_copy(n, dy):
        q = sta_at(n, dy)
        return pltpu.make_async_remote_copy(
            src_ref=raw_send.at[lax.rem(q, 8)], dst_ref=raw_recv.at[sj],
            send_sem=raw_ss, recv_sem=raw_rs.at[n // 2],
            device_id=(bi, q), device_id_type=MESH,
        )

    def tot_copy(n, dy):
        return pltpu.make_async_remote_copy(
            src_ref=tot_send, dst_ref=tot_recv.at[sj],
            send_sem=tot_ss, recv_sem=tot_rs.at[n],
            device_id=(bi, sta_at(n, dy)), device_id_type=MESH,
        )

    def forward_copy(n):
        block = tot_recv.at[pl.ds(rows[n] * 4, 4)]
        return pltpu.make_async_remote_copy(
            src_ref=block, dst_ref=block, send_sem=forward_ss, recv_sem=tot_rs.at[n],
            device_id=(chip, sj), device_id_type=MESH,
        )

    def send_raw(n):
        for dy in FAR_Y:
            if (n, dy) != (0, 0):
                raw_copy(n, dy).start()

    def send_tot(n):
        for dy in FAR_Y:
            if (n, dy) != (0, 0):
                tot_copy(n, dy).start()

    def pow_copy(d):
        m = lax.rem(own + d, 8)
        return pltpu.make_async_remote_copy(
            src_ref=pow_send.at[m], dst_ref=pow_recv.at[own],
            send_sem=pow_ss, recv_sem=pow_rs,
            device_id=(bi, pair * 8 + m), device_id_type=MESH,
        )

    def wait_all(buf, count, sem):
        blocks = buf.at[pl.ds(0, count)]
        pltpu.make_async_copy(blocks, blocks, sem).wait()

    with scope("d_barrier"):
        @pl.when(early & (core == 1))
        def _():
            pl.semaphore_wait(barrier, 21)

        @pl.when(late & (core == 1))
        def _():
            pl.semaphore_wait(barrier, 30)

        @pl.when(core == 0)
        def _():
            pl.semaphore_wait(barrier, 1)
            side_copy.start()

    with scope("e_side"):
        @pl.when(core == 1)
        def _():
            side_copy.wait_recv()
            part = (side + side_recv[...]).astype(jnp.bfloat16)
            part_send[...] = part
            for n in range(7):
                part_copy(n).start()
            go(0)
            part_recv[lax.div(bi, 2)] = part

            def announce(first, last):
                def one(q):
                    @pl.when(q != sj)
                    def _():
                        pl.semaphore_signal(late_sem, inc=1, device_id=(bi, q), device_id_type=MESH)

                loop(first, last, one)

            @pl.when(late)
            def _():
                announce(0, 16)

        @pl.when(core == 0)
        def _():
            pl.semaphore_wait(go_sem.at[0], 1)

    with scope("e_send1"):
        @pl.when(late)
        def _():
            send_raw(3)
            send_raw(2)

        @pl.when(early)
        def _():
            send_raw(1)
            send_raw(0)

        raw_recv[sj] = raw_send[own]

    loads[1].wait()
    loads[2].wait()
    row8 = iota((8, 256), 0)
    odd32 = iota((32, 256), 0) * 2 + 1
    coarse = row8 * 8 + 4
    fine = jnp.where(row8 == 0, 1, 3)

    def tables(j):
        lanes = pl.ds(pl.multiple_of(j * 256, 256), 256)
        cx = cov[0:1, lanes] * f1
        cy = cov[1:2, lanes] * f1
        c, s = cos_sin(coarse * cx)
        tabc[0, :, lanes] = c
        tabc[1, :, lanes] = s
        c, s = cos_sin(jnp.where(row8 < 2, fine * cx, jnp.broadcast_to(cx + cy, (8, 256))))
        tabr[0, :, lanes] = c
        tabr[1, :, lanes] = s
        cyt, syt = cos_sin(odd32 * cy)
        cols = []
        for trig in range(2):
            for tab in (cyt, syt):
                for f in range(2):
                    cols.append(tabr[trig, f : f + 1, lanes] * tab)
        tabt[lanes, :] = jnp.concatenate(cols, 0).astype(jnp.bfloat16).T

    with scope("f_tables"):
        loop(0, 16, tables)

    @pl.when(core == 1)
    def _():
        with scope("g_partwait"):
            wait_all(part_recv, 7, part_rs)
        with scope("h_total"):
            total = part_recv[0].astype(jnp.float32)
            for p in range(1, 8):
                total = total + part_recv[p].astype(jnp.float32)
            total = total.astype(jnp.bfloat16)
            tot_send[...] = total

            @pl.when(late)
            def _():
                send_tot(3)
                send_tot(2)

            @pl.when(early)
            def _():
                send_tot(1)
                send_tot(0)

            tot_recv[sj] = total

    with scope("i_pick"):
        beams = pl.ds(pl.multiple_of(pair * 1024, 1024), 1024)
        sx = slv[0:1, beams]
        sy = slv[1:2, beams]
        u = sx + 32
        m = lax.shift_right_arithmetic(u, 2)
        f = u & 3
        cpos = m >= 8
        fpos = f >= 2
        ypos = sy >= 0
        cidx = jnp.where(cpos, m - 8, 7 - m)
        fidx = jnp.where(fpos, f - 2, 1 - f)
        ky = jnp.where(ypos, sy, -1 - sy)
        c01 = jnp.where(cpos, 1, 0)
        rel = jnp.where(c01 == jnp.where(fpos, 1, 0), 0, 1)
        diff = jnp.where(c01 == jnp.where(ypos, 1, 0), 0, 1)
        pick_row = (rel * 2 + diff) * 8 + cidx
        pick_col = (1 - c01) * 64 + fidx * 32 + ky
    with scope("i_late"):
        @pl.when(early & (core == 1))
        def _():
            pl.semaphore_wait(late_sem, 8)
            go(1)
            send_tot(2)
            send_tot(3)

        @pl.when(late & (core == 1))
        def _():
            pl.semaphore_wait(late_sem, 7)
            go(1)
            send_tot(1)
            send_tot(0)

        @pl.when(core == 0)
        def _():
            pl.semaphore_wait(go_sem.at[1], 1)

        @pl.when(early)
        def _():
            send_raw(2)
            send_raw(3)

        @pl.when(late)
        def _():
            send_raw(1)
            send_raw(0)

    def rotate(n):
        def block(y):
            j = rows[n] * 4 + y
            lanes = pl.ds(pl.multiple_of(j * 256, 256), 256)
            raw = raw_recv[j].astype(jnp.float32)
            re = jnp.concatenate([raw[:8], raw[16:24]], 1)
            im = jnp.concatenate([raw[8:16], raw[24:]], 1)
            c = tabr[0, 2:3, lanes]
            s = tabr[1, 2:3, lanes]
            xrot[0:8, lanes] = re * c - im * s
            xrot[8:16, lanes] = im * c + re * s

        loop(0, 4, block)

    for n in range(4):
        if n % 2 == 0:
            with scope("j_rawwait"):
                wait_all(raw_recv, 7 + n // 2, raw_rs.at[n // 2])
            with scope("k_rotate"):
                rotate(n)
                rotate(n + 1)
        with scope("l_totwait%d" % n):
            @pl.when(core == 0)
            def _(n=n):
                wait_all(tot_recv, 4, tot_rs.at[n])

            @pl.when(core == 1)
            def _(n=n):
                wait_all(tot_recv, 4 if n else 3, tot_rs.at[n])
                forward_copy(n).start()
        with scope("m_main"):
            lanes = pl.ds(pl.multiple_of(rows[n] * 1024, 1024), 1024)
            at = slice(n * 1024, n * 1024 + 1024)
            parts = []
            for y in range(4):
                total = tot_recv[rows[n] * 4 + y].astype(jnp.float32)
                parts += [total[:8], total[8:]]
            inv = lax.rsqrt(jnp.concatenate(parts, 1) * (1.0 / 256) + epsilon)
            wbuf[0:8, at] = xrot[0:8, lanes] * inv
            wbuf[8:16, at] = xrot[8:16, lanes] * inv
            v = []
            for trig in range(2):
                tab = tabc[trig, :, lanes]
                for row in range(16):
                    v.append(wbuf[row : row + 1, at] * tab)
            acc = jnp.dot(
                jnp.concatenate(v, 0).astype(jnp.bfloat16), tabt[lanes, :], preferred_element_type=jnp.float32
            )
            if n == 0:
                accum[...] = acc
            elif n < 3:
                accum[...] += acc
            else:
                acc = acc + accum[...]

    with scope("n_post"):
        mark = jnp.where(iota((128, 128), 1) < 64, -1.0, 1.0)
        cc, cs, sc, ss = acc[:128, :128], acc[:128, 128:], acc[128:, :128], acc[128:, 128:]
        grid = []

        def seg_sum(a):
            a = a * a
            total = a[:8]
            for g in range(1, 8):
                total = total + a[8 * g : 8 * g + 8]
            return total

        for x, y in ((cc - ss, sc + cs), (cc + ss, sc - cs)):
            y = pltpu.roll(y, 64, 1) * mark
            plus, minus = x + y, x - y
            turned = pltpu.roll(plus[64:], 64, 1)
            grid.append(seg_sum(plus[:64] + turned) + pltpu.roll(seg_sum(plus[:64] - turned), 64, 1))
            turned = pltpu.roll(minus[64:], 64, 1)
            grid.append(seg_sum(minus[:64] - turned) + pltpu.roll(seg_sum(minus[:64] + turned), 64, 1))
        grid = jnp.concatenate(grid, 0) * (1.0 / 32768)
        row = iota((8, 128), 0)
        for n in range(8):
            at = slice(128 * n, 128 * n + 128)
            col = jnp.broadcast_to(pick_col[:, at], (8, 128))
            hit = jnp.broadcast_to(pick_row[:, at], (8, 128))
            total = jnp.zeros((8, 128), jnp.float32)
            for k in range(4):
                values = jnp.take_along_axis(grid[8 * k : 8 * k + 8], col, axis=1)
                total = total + jnp.where(row + 8 * k == hit, values, 0.0)
            pow_send[n] = jnp.sum(total, 0, keepdims=True)
    with scope("o_powsend"):
        for d in range(7, 0, -1):
            pow_copy(d).start()
        pow_recv[own] = pow_send[own]

    with scope("p_sendwait"):
        @pl.when(core == 0)
        def _():
            side_copy.wait_send()

        @pl.when(core == 1)
        def _():
            wait_all(part_recv, 7, part_ss)
            wait_all(tot_recv, 15, tot_ss)
            wait_all(tot_recv, 16, forward_ss)

        wait_all(raw_recv, 15, raw_ss)

    with scope("q_powwait"):
        wait_all(pow_recv, 7, pow_rs)

    with scope("r_end"):
        for b in range(8):
            out_ref[b : b + 1, :] = pow_recv[b]
        wait_all(pow_recv, 7, pow_ss)


def local(spectra, coords, slowness):
    f32, bf16, i32 = jnp.float32, jnp.bfloat16, jnp.int32
    dma = pltpu.SemaphoreType.DMA
    return pl.pallas_call(
        kernel,
        out_shape=jax.ShapeDtypeStruct((8, 128), f32),
        in_specs=[pl.BlockSpec(memory_space=pl.ANY)] * 3,
        out_specs=pl.BlockSpec(memory_space=pltpu.VMEM),
        scratch_shapes=[
            pltpu.VMEM((2, 8, 8, 256), bf16),
            pltpu.VMEM((2, 4096), i32),
            pltpu.VMEM((2, 2048), i32),
            pltpu.VMEM((8, 32, 128), bf16),
            pltpu.VMEM((16, 32, 128), bf16),
            pltpu.VMEM((16, 128), f32),
            pltpu.VMEM((16, 128), f32),
            pltpu.VMEM((16, 128), bf16),
            pltpu.VMEM((8, 16, 128), bf16),
            pltpu.VMEM((16, 128), bf16),
            pltpu.VMEM((16, 16, 128), bf16),
            pltpu.VMEM((8, 1, 128), f32),
            pltpu.VMEM((8, 1, 128), f32),
            pltpu.VMEM((2, 8, 4096), f32),
            pltpu.VMEM((4096, 256), bf16),
            pltpu.VMEM((2, 8, 4096), f32),
            pltpu.VMEM((16, 4096), f32),
            pltpu.VMEM((16, 4096), f32),
            pltpu.VMEM((256, 256), f32),
            dma((3,)),
            pltpu.SemaphoreType.REGULAR,
            pltpu.SemaphoreType.REGULAR((2,)),
            dma, dma,
            dma, dma, dma, dma((2,)), dma, dma((4,)), dma, dma, dma,
        ],
        compiler_params=pltpu.CompilerParams(
            collective_id=0, has_side_effects=True, vmem_limit_bytes=56540000
        ),
    )(spectra, coords, slowness)


def solution(mesh):
    in_specs = (P(None, "bins", None, "sta"), P(), P())
    out_specs = P("bins", "sta")
    return jax.shard_map(local, mesh=mesh, in_specs=in_specs, out_specs=out_specs, check_vma=False)
```

```python
import jax
import jax.numpy as jnp
import numpy as np
from jax import lax
from jax.experimental import pallas as pl
from jax.experimental.pallas import tpu as pltpu
from jax.sharding import PartitionSpec as P

MESH = pl.DeviceIdType.MESH
epsilon = 1e-06
scope = jax.named_scope

FAR_Y = (2, 1, 3, 0)
FAR_BINS = sorted(((dx, dl) for dx in range(4) for dl in range(2)), key=lambda o: -min(o[0], 4 - o[0]) - o[1])


def cheb_fit(fn, degree):
    nodes = np.cos(np.pi * (np.arange(4001) + 0.5) / 4001)
    u = (nodes + 1.0) / 2.0
    return np.polynomial.chebyshev.Chebyshev.fit(u, fn(u), degree, domain=[0, 1]).convert(
        kind=np.polynomial.Polynomial
    ).coef


COS = [float(c) for c in cheb_fit(lambda u: np.cos(np.pi * np.sqrt(u)), 7)]
SIN = [float(c) for c in cheb_fit(lambda u: np.pi * np.sinc(np.sqrt(u)), 6)]


def horner(coefs, u):
    acc = jnp.full_like(u, coefs[-1])
    for c in coefs[-2::-1]:
        acc = acc * u + c
    return acc


def cos_sin(index):
    t = lax.shift_right_arithmetic(lax.shift_left(index, 11), 11).astype(jnp.float32) * (1.0 / 1048576)
    u = t * t
    return horner(COS, u), horner(SIN, u) * t


def iota(shape, dim):
    return lax.broadcasted_iota(jnp.int32, shape, dim)


def kernel(
    x_hbm, co_hbm, sl_hbm, out_ref,
    xv, cov, slv, raw_send, raw_recv, more_recv, side_send, side_recv, part_send, part_recv, tot_send, tot_recv, pow_send, pow_recv,
    tabc, tabt, tabr, xrot, wbuf, accum,
    tabc2, tabt2, tabr2, xrot2, wbuf2, accum2,
    in_sem, late_sem, go_sem, side_ss, side_rs, part_ss, part_rs, raw_ss, more_ss, raw_rs, tot_ss, tot_rs, forward_ss, pow_ss, pow_rs,
):
    bi = lax.axis_index("bins")
    sj = lax.axis_index("sta")
    core = lax.rem(bi, 2)
    chip = bi - core
    px = lax.div(bi, 4)
    pl_lo = lax.rem(lax.div(bi, 2), 2)
    pz = lax.div(sj, 4)
    py = lax.rem(sj, 4)
    pair = lax.div(sj, 8)
    own = lax.rem(sj, 8)
    f1 = bi * 8 + own + 1

    early = pz < 2
    late = pz >= 2
    first_row = (pz == 0) & (pl_lo == 0)
    next_row = (pz == 1) & (pl_lo == 0)
    plain = (pz >= 2) | (pl_lo == 1)
    rows = (pz, pz + 1 - 2 * lax.rem(pz, 2), 3 - pz, lax.rem(pz + 2, 4))

    def sta_at(n, dy):
        return rows[n] * 4 + lax.rem(py + dy, 4)

    def chip_at(o):
        return lax.rem(px + o[0], 4) * 4 + lax.rem(pl_lo + o[1], 2) * 2

    loads = [
        pltpu.make_async_copy(src, dst, in_sem.at[n])
        for n, (src, dst) in enumerate(((x_hbm, xv), (co_hbm, cov), (sl_hbm, slv)))
    ]
    for load in loads:
        load.start()

    barrier = pltpu.get_barrier_semaphore()

    def greet(b, s):
        pl.semaphore_signal(barrier, inc=1, device_id=(b, s), device_id_type=MESH)

    def loop(lo, hi, body):
        lax.fori_loop(lo, hi, lambda d, c: (body(d), c)[1], 0)

    with scope("a_greet"):
        @pl.when(core == 1)
        def _():
            greet(chip, sj)
            for o in FAR_BINS[:7]:
                greet(chip_at(o) + 1, sj)

            @pl.when(early)
            def _():
                loop(1, 16, lambda d: greet(bi, lax.rem(sj + d, 16)))

            @pl.when(late)
            def _():
                loop(1, 8, lambda d: greet(bi, 8 + lax.rem(sj + d, 8)))

        @pl.when(early & (core == 0))
        def _():
            loop(1, 16, lambda d: greet(chip + 1, lax.rem(sj + d, 16)))

    with scope("b_xwait"):
        loads[0].wait()

    with scope("c_sumsq"):
        sq = jnp.zeros((8, 256), jnp.float32)
        for b in range(8):
            re = xv[0, b].astype(jnp.float32)
            im = xv[1, b].astype(jnp.float32)
            sq = sq + (re * re + im * im)
            raw_send[b] = jnp.concatenate(
                [re[:, :128], im[:, :128], re[:, 128:], im[:, 128:]], 0
            ).astype(jnp.bfloat16)
        side = jnp.concatenate([sq[:, :128], sq[:, 128:]], 0)
        side_send[...] = side

    side_copy = pltpu.make_async_remote_copy(
        src_ref=side_send, dst_ref=side_recv, send_sem=side_ss, recv_sem=side_rs,
        device_id=(chip + 1, sj), device_id_type=MESH,
    )

    def go(n):
        pl.semaphore_signal(go_sem.at[n], inc=1, device_id=(chip, sj), device_id_type=MESH)

    def part_copy(n):
        return pltpu.make_async_remote_copy(
            src_ref=part_send, dst_ref=part_recv.at[lax.div(bi, 2)],
            send_sem=part_ss, recv_sem=part_rs,
            device_id=(chip_at(FAR_BINS[n]) + 1, sj), device_id_type=MESH,
        )

    def raw_copy(n, dy):
        q = sta_at(n, dy)
        return pltpu.make_async_remote_copy(
            src_ref=raw_send.at[lax.rem(q, 8)], dst_ref=raw_recv.at[sj],
            send_sem=raw_ss, recv_sem=raw_rs.at[n // 2],
            device_id=(bi, q), device_id_type=MESH,
        )

    def tot_copy(n, dy):
        return pltpu.make_async_remote_copy(
            src_ref=tot_send, dst_ref=tot_recv.at[sj],
            send_sem=tot_ss, recv_sem=tot_rs.at[n],
            device_id=(bi, sta_at(n, dy)), device_id_type=MESH,
        )

    def forward_copy(n):
        block = tot_recv.at[pl.ds(rows[n] * 4, 4)]
        return pltpu.make_async_remote_copy(
            src_ref=block, dst_ref=block, send_sem=forward_ss, recv_sem=tot_rs.at[n],
            device_id=(chip, sj), device_id_type=MESH,
        )

    def more_copy(n, dy):
        q = sta_at(n, dy)
        return pltpu.make_async_remote_copy(
            src_ref=raw_send.at[lax.rem(q, 4) + 4], dst_ref=more_recv.at[sj],
            send_sem=more_ss, recv_sem=raw_rs.at[n // 2],
            device_id=(bi, q), device_id_type=MESH,
        )

    def send_raw(n):
        for dy in FAR_Y:
            if (n, dy) != (0, 0):
                raw_copy(n, dy).start()

        @pl.when((pz == (0, 1, 3, 2)[n]) & (pl_lo == 0))
        def _():
            for dy in FAR_Y:
                if (n, dy) != (0, 0):
                    more_copy(n, dy).start()

    def send_tot(n):
        for dy in FAR_Y:
            if (n, dy) != (0, 0):
                tot_copy(n, dy).start()

    def pow_copy(tile, m, slot):
        return pltpu.make_async_remote_copy(
            src_ref=pow_send.at[tile], dst_ref=pow_recv.at[slot],
            send_sem=pow_ss, recv_sem=pow_rs,
            device_id=(bi, pair * 8 + m), device_id_type=MESH,
        )

    def wait_all(buf, count, sem):
        blocks = buf.at[pl.ds(0, count)]
        pltpu.make_async_copy(blocks, blocks, sem).wait()

    with scope("d_barrier"):
        @pl.when(early & (core == 1))
        def _():
            pl.semaphore_wait(barrier, 21)

        @pl.when(late & (core == 1))
        def _():
            pl.semaphore_wait(barrier, 30)

        @pl.when(core == 0)
        def _():
            pl.semaphore_wait(barrier, 1)
            side_copy.start()

    with scope("e_side"):
        @pl.when(core == 1)
        def _():
            side_copy.wait_recv()
            part = (side + side_recv[...]).astype(jnp.bfloat16)
            part_send[...] = part
            for n in range(7):
                part_copy(n).start()
            go(0)
            part_recv[lax.div(bi, 2)] = part

            def announce(first, last):
                def one(q):
                    @pl.when(q != sj)
                    def _():
                        pl.semaphore_signal(late_sem, inc=1, device_id=(bi, q), device_id_type=MESH)

                loop(first, last, one)

            @pl.when(late)
            def _():
                announce(0, 16)

        @pl.when(core == 0)
        def _():
            pl.semaphore_wait(go_sem.at[0], 1)

    with scope("e_send1"):
        @pl.when(late)
        def _():
            send_raw(3)
            send_raw(2)

        @pl.when(early)
        def _():
            send_raw(1)
            send_raw(0)

        raw_recv[sj] = raw_send[own]

        @pl.when(first_row)
        def _():
            more_recv[sj] = raw_send[own + 4]

    loads[1].wait()
    loads[2].wait()
    row8 = iota((8, 256), 0)
    odd32 = iota((32, 256), 0) * 2 + 1
    coarse = row8 * 8 + 4
    fine = jnp.where(row8 == 0, 1, 3)

    def tables(j, f, tabc, tabt, tabr):
        lanes = pl.ds(pl.multiple_of(j * 256, 256), 256)
        cx = cov[0:1, lanes] * f
        cy = cov[1:2, lanes] * f
        c, s = cos_sin(coarse * cx)
        tabc[0, :, lanes] = c
        tabc[1, :, lanes] = s
        c, s = cos_sin(jnp.where(row8 < 2, fine * cx, jnp.broadcast_to(cx + cy, (8, 256))))
        tabr[0, :, lanes] = c
        tabr[1, :, lanes] = s
        cyt, syt = cos_sin(odd32 * cy)
        cols = []
        for trig in range(2):
            for tab in (cyt, syt):
                for k in range(2):
                    cols.append(tabr[trig, k : k + 1, lanes] * tab)
        tabt[lanes, :] = jnp.concatenate(cols, 0).astype(jnp.bfloat16).T

    with scope("f_tables"):
        loop(0, 16, lambda j: tables(j, f1, tabc, tabt, tabr))

        @pl.when(first_row)
        def _():
            loop(0, 16, lambda j: tables(j, f1 + 4, tabc2, tabt2, tabr2))

    @pl.when(core == 1)
    def _():
        with scope("g_partwait"):
            wait_all(part_recv, 7, part_rs)
        with scope("h_total"):
            total = part_recv[0].astype(jnp.float32)
            for p in range(1, 8):
                total = total + part_recv[p].astype(jnp.float32)
            total = total.astype(jnp.bfloat16)
            tot_send[...] = total

            @pl.when(late)
            def _():
                send_tot(3)
                send_tot(2)

            @pl.when(early)
            def _():
                send_tot(1)
                send_tot(0)

            tot_recv[sj] = total

    with scope("i_pick"):
        beams = pl.ds(pl.multiple_of(pair * 1024, 1024), 1024)
        sx = slv[0:1, beams]
        sy = slv[1:2, beams]
        u = sx + 32
        m = lax.shift_right_arithmetic(u, 2)
        f = u & 3
        cpos = m >= 8
        fpos = f >= 2
        ypos = sy >= 0
        cidx = jnp.where(cpos, m - 8, 7 - m)
        fidx = jnp.where(fpos, f - 2, 1 - f)
        ky = jnp.where(ypos, sy, -1 - sy)
        c01 = jnp.where(cpos, 1, 0)
        rel = jnp.where(c01 == jnp.where(fpos, 1, 0), 0, 1)
        diff = jnp.where(c01 == jnp.where(ypos, 1, 0), 0, 1)
        pick_row = (rel * 2 + diff) * 8 + cidx
        pick_col = (1 - c01) * 64 + fidx * 32 + ky
    with scope("i_late"):
        @pl.when(early & (core == 1))
        def _():
            pl.semaphore_wait(late_sem, 8)
            go(1)
            send_tot(2)
            send_tot(3)

        @pl.when(late & (core == 1))
        def _():
            pl.semaphore_wait(late_sem, 7)
            go(1)
            send_tot(1)
            send_tot(0)

        @pl.when(core == 0)
        def _():
            pl.semaphore_wait(go_sem.at[1], 1)

        @pl.when(early)
        def _():
            send_raw(2)
            send_raw(3)

        @pl.when(late)
        def _():
            send_raw(1)
            send_raw(0)

    first = (raw_recv, tabc, tabt, tabr, xrot, wbuf, accum)
    second = (more_recv, tabc2, tabt2, tabr2, xrot2, wbuf2, accum2)

    def rotate(n, bufs):
        raw_recv, tabc, tabt, tabr, xrot, wbuf, accum = bufs

        def block(y):
            j = rows[n] * 4 + y
            lanes = pl.ds(pl.multiple_of(j * 256, 256), 256)
            raw = raw_recv[j].astype(jnp.float32)
            re = jnp.concatenate([raw[:8], raw[16:24]], 1)
            im = jnp.concatenate([raw[8:16], raw[24:]], 1)
            c = tabr[0, 2:3, lanes]
            s = tabr[1, 2:3, lanes]
            xrot[0:8, lanes] = re * c - im * s
            xrot[8:16, lanes] = im * c + re * s

        loop(0, 4, block)

    def scales(n):
        parts = []
        for y in range(4):
            total = tot_recv[rows[n] * 4 + y].astype(jnp.float32)
            parts += [total[:8], total[8:]]
        return lax.rsqrt(jnp.concatenate(parts, 1) * (1.0 / 256) + epsilon)

    def amplitudes(n, inv, bufs):
        raw_recv, tabc, tabt, tabr, xrot, wbuf, accum = bufs
        lanes = pl.ds(pl.multiple_of(rows[n] * 1024, 1024), 1024)
        at = slice(n * 1024, n * 1024 + 1024)
        wbuf[0:8, at] = xrot[0:8, lanes] * inv
        wbuf[8:16, at] = xrot[8:16, lanes] * inv
        v = []
        for trig in range(2):
            tab = tabc[trig, :, lanes]
            for row in range(16):
                v.append(wbuf[row : row + 1, at] * tab)
        acc = jnp.dot(
            jnp.concatenate(v, 0).astype(jnp.bfloat16), tabt[lanes, :], preferred_element_type=jnp.float32
        )
        if n == 3:
            return acc + accum[...]
        if n == 0:
            accum[...] = acc
        else:
            accum[...] += acc

    def powers(acc):
        cc, cs, sc, ss = acc[:128, :128], acc[:128, 128:], acc[128:, :128], acc[128:, 128:]
        grid = []

        def seg_sum(a):
            a = a * a
            total = a[:8]
            for g in range(1, 8):
                total = total + a[8 * g : 8 * g + 8]
            return total

        for x, y in ((cc - ss, sc + cs), (cc + ss, sc - cs)):
            y = pltpu.roll(y, 64, 1) * mark
            plus, minus = x + y, x - y
            turned = pltpu.roll(plus[64:], 64, 1)
            grid.append(seg_sum(plus[:64] + turned) + pltpu.roll(seg_sum(plus[:64] - turned), 64, 1))
            turned = pltpu.roll(minus[64:], 64, 1)
            grid.append(seg_sum(minus[:64] - turned) + pltpu.roll(seg_sum(minus[:64] + turned), 64, 1))
        return jnp.concatenate(grid, 0) * (1.0 / 32768)

    def pick(grid, tiles, base):
        row = iota((8, 128), 0)
        for n in range(tiles):
            at = slice(128 * n, 128 * n + 128)
            col = jnp.broadcast_to(pick_col[:, at], (8, 128))
            hit = jnp.broadcast_to(pick_row[:, at], (8, 128))
            total = jnp.zeros((8, 128), jnp.float32)
            for k in range(4):
                values = jnp.take_along_axis(grid[8 * k : 8 * k + 8], col, axis=1)
                total = total + jnp.where(row + 8 * k == hit, values, 0.0)
            pow_send[base + n] = jnp.sum(total, 0, keepdims=True)

    mark = jnp.where(iota((128, 128), 1) < 64, -1.0, 1.0)

    for n in range(4):
        if n % 2 == 0:
            with scope("j_rawwait"):
                @pl.when(first_row)
                def _(n=n):
                    wait_all(raw_recv, 14 + n, raw_rs.at[n // 2])

                @pl.when(next_row | plain)
                def _(n=n):
                    wait_all(raw_recv, 7 + n // 2, raw_rs.at[n // 2])

            with scope("k_rotate"):
                rotate(n, first)
                rotate(n + 1, first)

                @pl.when(first_row)
                def _(n=n):
                    rotate(n, second)
                    rotate(n + 1, second)

        with scope("l_totwait%d" % n):
            @pl.when(core == 0)
            def _(n=n):
                wait_all(tot_recv, 4, tot_rs.at[n])

            @pl.when(core == 1)
            def _(n=n):
                wait_all(tot_recv, 4 if n else 3, tot_rs.at[n])
                forward_copy(n).start()

        with scope("m_main"):
            @pl.when(first_row)
            def _(n=n):
                inv = scales(n)
                acc = amplitudes(n, inv, first)
                acc2 = amplitudes(n, inv, second)
                if n == 3:
                    pick(powers(acc2), 4, 8)
                    pick(powers(acc), 8, 0)

            @pl.when(next_row | plain)
            def _(n=n):
                acc = amplitudes(n, scales(n), first)
                if n == 3:
                    pick(powers(acc), 8, 0)

    with scope("o_powsend"):
        @pl.when(first_row)
        def _():
            for dy in (2, 1, 3):
                m = lax.rem(own + dy, 4)
                pow_copy(8 + m, m, own + 4).start()
                pow_copy(m, m, own).start()
            for y in range(4, 8):
                pow_copy(y, y, own).start()
            pow_recv[own + 4] = pow_send[8 + own]

        @pl.when(next_row)
        def _():
            for dy in (2, 1, 3):
                m = 4 + lax.rem(own + dy, 4)
                pow_copy(m, m, own).start()

        @pl.when(plain)
        def _():
            for d in range(7, 0, -1):
                m = lax.rem(own + d, 8)
                pow_copy(m, m, own).start()

        pow_recv[own] = pow_send[own]

    with scope("p_sendwait"):
        @pl.when(core == 0)
        def _():
            side_copy.wait_send()

        @pl.when(core == 1)
        def _():
            wait_all(part_recv, 7, part_ss)
            wait_all(tot_recv, 15, tot_ss)
            wait_all(tot_recv, 16, forward_ss)

        wait_all(raw_recv, 15, raw_ss)

        @pl.when(first_row)
        def _():
            wait_all(more_recv, 3, more_ss)

        @pl.when((pz > 0) & (pl_lo == 0))
        def _():
            wait_all(more_recv, 4, more_ss)

    with scope("q_powwait"):
        @pl.when(first_row)
        def _():
            wait_all(pow_send, 6, pow_rs)

        @pl.when(next_row | plain)
        def _():
            wait_all(pow_send, 7, pow_rs)

    with scope("r_end"):
        for b in range(8):
            out_ref[b : b + 1, :] = pow_recv[b]
        for row, count in ((first_row, 10), (next_row, 3), (plain, 7)):
            @pl.when(row)
            def _(count=count):
                wait_all(pow_send, count, pow_ss)


def local(spectra, coords, slowness):
    f32, bf16, i32 = jnp.float32, jnp.bfloat16, jnp.int32
    dma = pltpu.SemaphoreType.DMA
    return pl.pallas_call(
        kernel,
        out_shape=jax.ShapeDtypeStruct((8, 128), f32),
        in_specs=[pl.BlockSpec(memory_space=pl.ANY)] * 3,
        out_specs=pl.BlockSpec(memory_space=pltpu.VMEM),
        scratch_shapes=[
            pltpu.VMEM((2, 8, 8, 256), bf16),
            pltpu.VMEM((2, 4096), i32),
            pltpu.VMEM((2, 2048), i32),
            pltpu.VMEM((8, 32, 128), bf16),
            pltpu.VMEM((16, 32, 128), bf16),
            pltpu.VMEM((16, 32, 128), bf16),
            pltpu.VMEM((16, 128), f32),
            pltpu.VMEM((16, 128), f32),
            pltpu.VMEM((16, 128), bf16),
            pltpu.VMEM((8, 16, 128), bf16),
            pltpu.VMEM((16, 128), bf16),
            pltpu.VMEM((16, 16, 128), bf16),
            pltpu.VMEM((12, 1, 128), f32),
            pltpu.VMEM((8, 1, 128), f32),
            pltpu.VMEM((2, 8, 4096), f32),
            pltpu.VMEM((4096, 256), bf16),
            pltpu.VMEM((2, 8, 4096), f32),
            pltpu.VMEM((16, 4096), f32),
            pltpu.VMEM((16, 4096), f32),
            pltpu.VMEM((256, 256), f32),
            pltpu.VMEM((2, 8, 4096), f32),
            pltpu.VMEM((4096, 256), bf16),
            pltpu.VMEM((2, 8, 4096), f32),
            pltpu.VMEM((16, 4096), f32),
            pltpu.VMEM((16, 4096), f32),
            pltpu.VMEM((256, 256), f32),
            dma((3,)),
            pltpu.SemaphoreType.REGULAR,
            pltpu.SemaphoreType.REGULAR((2,)),
            dma, dma,
            dma, dma, dma, dma, dma((2,)), dma, dma((4,)), dma, dma, dma,
        ],
        compiler_params=pltpu.CompilerParams(
            collective_id=0, has_side_effects=True, vmem_limit_bytes=56540000
        ),
    )(spectra, coords, slowness)


def solution(mesh):
    in_specs = (P(None, "bins", None, "sta"), P(), P())
    out_specs = P("bins", "sta")
    return jax.shard_map(local, mesh=mesh, in_specs=in_specs, out_specs=out_specs, check_vma=False)
```

```python
import jax
import jax.numpy as jnp
import numpy as np
from jax import lax
from jax.experimental import pallas as pl
from jax.experimental.pallas import tpu as pltpu
from jax.sharding import PartitionSpec as P

MESH = pl.DeviceIdType.MESH
epsilon = 1e-06
scope = jax.named_scope

FAR_Y = (2, 1, 3, 0)
FAR_BINS = sorted(((dx, dl) for dx in range(4) for dl in range(2)), key=lambda o: -min(o[0], 4 - o[0]) - o[1])


def cheb_fit(fn, degree):
    nodes = np.cos(np.pi * (np.arange(4001) + 0.5) / 4001)
    u = (nodes + 1.0) / 2.0
    return np.polynomial.chebyshev.Chebyshev.fit(u, fn(u), degree, domain=[0, 1]).convert(
        kind=np.polynomial.Polynomial
    ).coef


COS = [float(c) for c in cheb_fit(lambda u: np.cos(np.pi * np.sqrt(u)), 7)]
SIN = [float(c) for c in cheb_fit(lambda u: np.pi * np.sinc(np.sqrt(u)), 6)]


def horner(coefs, u):
    acc = jnp.full_like(u, coefs[-1])
    for c in coefs[-2::-1]:
        acc = acc * u + c
    return acc


def cos_sin(index):
    t = lax.shift_right_arithmetic(lax.shift_left(index, 11), 11).astype(jnp.float32) * (1.0 / 1048576)
    u = t * t
    return horner(COS, u), horner(SIN, u) * t


def iota(shape, dim):
    return lax.broadcasted_iota(jnp.int32, shape, dim)


def kernel(
    x_hbm, co_hbm, sl_hbm, out_ref,
    xv, cov, slv, raw_send, raw_recv, more_recv, side_send, side_recv, part_send, part_recv, tot_send, tot_recv, pow_send, pow_recv,
    tabc, tabt, tabr, xrot, wbuf, accum,
    tabc2, tabt2, tabr2, xrot2, wbuf2, accum2,
    in_sem, late_sem, go_sem, side_ss, side_rs, part_ss, part_rs, raw_ss, more_ss, raw_rs, tot_ss, tot_rs, forward_ss, pow_ss, pow_rs,
):
    bi = lax.axis_index("bins")
    sj = lax.axis_index("sta")
    core = lax.rem(bi, 2)
    chip = bi - core
    px = lax.div(bi, 4)
    pl_lo = lax.rem(lax.div(bi, 2), 2)
    pz = lax.div(sj, 4)
    py = lax.rem(sj, 4)
    pair = lax.div(sj, 8)
    own = lax.rem(sj, 8)
    f1 = bi * 8 + own + 1

    early = pz < 2
    late = pz >= 2
    first_row = (pz == 0) & (pl_lo == 0)
    next_row = (pz == 1) & (pl_lo == 0)
    plain = (pz >= 2) | (pl_lo == 1)
    rows = (pz, pz + 1 - 2 * lax.rem(pz, 2), 3 - pz, lax.rem(pz + 2, 4))

    def sta_at(n, dy):
        return rows[n] * 4 + lax.rem(py + dy, 4)

    def chip_at(o):
        return lax.rem(px + o[0], 4) * 4 + lax.rem(pl_lo + o[1], 2) * 2

    loads = [
        pltpu.make_async_copy(src, dst, in_sem.at[n])
        for n, (src, dst) in enumerate(((x_hbm, xv), (co_hbm, cov), (sl_hbm, slv)))
    ]
    for load in loads:
        load.start()

    barrier = pltpu.get_barrier_semaphore()

    def greet(b, s):
        pl.semaphore_signal(barrier, inc=1, device_id=(b, s), device_id_type=MESH)

    def loop(lo, hi, body):
        lax.fori_loop(lo, hi, lambda d, c: (body(d), c)[1], 0)

    with scope("a_greet"):
        @pl.when(core == 1)
        def _():
            greet(chip, sj)
            for o in FAR_BINS[:7]:
                greet(chip_at(o) + 1, sj)

            @pl.when(early)
            def _():
                loop(1, 16, lambda d: greet(bi, lax.rem(sj + d, 16)))

            @pl.when(late)
            def _():
                loop(1, 8, lambda d: greet(bi, 8 + lax.rem(sj + d, 8)))

        @pl.when(early & (core == 0))
        def _():
            loop(1, 16, lambda d: greet(chip + 1, lax.rem(sj + d, 16)))

    with scope("b_xwait"):
        loads[0].wait()

    with scope("c_sumsq"):
        sq = jnp.zeros((8, 256), jnp.float32)
        for b in range(8):
            re = xv[0, b].astype(jnp.float32)
            im = xv[1, b].astype(jnp.float32)
            sq = sq + (re * re + im * im)
            raw_send[b] = jnp.concatenate(
                [re[:, :128], im[:, :128], re[:, 128:], im[:, 128:]], 0
            ).astype(jnp.bfloat16)
        side = jnp.concatenate([sq[:, :128], sq[:, 128:]], 0)
        side_send[...] = side

    side_copy = pltpu.make_async_remote_copy(
        src_ref=side_send, dst_ref=side_recv, send_sem=side_ss, recv_sem=side_rs,
        device_id=(chip + 1, sj), device_id_type=MESH,
    )

    def go(n):
        pl.semaphore_signal(go_sem.at[n], inc=1, device_id=(chip, sj), device_id_type=MESH)

    def part_copy(n):
        return pltpu.make_async_remote_copy(
            src_ref=part_send, dst_ref=part_recv.at[lax.div(bi, 2)],
            send_sem=part_ss, recv_sem=part_rs,
            device_id=(chip_at(FAR_BINS[n]) + 1, sj), device_id_type=MESH,
        )

    def raw_copy(n, dy):
        q = sta_at(n, dy)
        return pltpu.make_async_remote_copy(
            src_ref=raw_send.at[lax.rem(q, 8)], dst_ref=raw_recv.at[sj],
            send_sem=raw_ss, recv_sem=raw_rs.at[n // 2],
            device_id=(bi, q), device_id_type=MESH,
        )

    def tot_copy(n, dy):
        return pltpu.make_async_remote_copy(
            src_ref=tot_send, dst_ref=tot_recv.at[sj],
            send_sem=tot_ss, recv_sem=tot_rs.at[n],
            device_id=(bi, sta_at(n, dy)), device_id_type=MESH,
        )

    def forward_copy(n):
        block = tot_recv.at[pl.ds(rows[n] * 4, 4)]
        return pltpu.make_async_remote_copy(
            src_ref=block, dst_ref=block, send_sem=forward_ss, recv_sem=tot_rs.at[n],
            device_id=(chip, sj), device_id_type=MESH,
        )

    def more_copy(n, dy):
        q = sta_at(n, dy)
        return pltpu.make_async_remote_copy(
            src_ref=raw_send.at[lax.rem(q, 4) + 4], dst_ref=more_recv.at[sj],
            send_sem=more_ss, recv_sem=raw_rs.at[n // 2],
            device_id=(bi, q), device_id_type=MESH,
        )

    def send_raw(n):
        for dy in FAR_Y:
            if (n, dy) != (0, 0):
                raw_copy(n, dy).start()

        @pl.when((pz == (0, 1, 3, 2)[n]) & (pl_lo == 0))
        def _():
            for dy in FAR_Y:
                if (n, dy) != (0, 0):
                    more_copy(n, dy).start()

    def send_tot(n):
        for dy in FAR_Y:
            if (n, dy) != (0, 0):
                tot_copy(n, dy).start()

    def pow_copy(tile, m, slot):
        return pltpu.make_async_remote_copy(
            src_ref=pow_send.at[tile], dst_ref=pow_recv.at[slot],
            send_sem=pow_ss, recv_sem=pow_rs,
            device_id=(bi, pair * 8 + m), device_id_type=MESH,
        )

    def wait_all(buf, count, sem):
        blocks = buf.at[pl.ds(0, count)]
        pltpu.make_async_copy(blocks, blocks, sem).wait()

    with scope("d_barrier"):
        @pl.when(early & (core == 1))
        def _():
            pl.semaphore_wait(barrier, 21)

        @pl.when(late & (core == 1))
        def _():
            pl.semaphore_wait(barrier, 30)

        @pl.when(core == 0)
        def _():
            pl.semaphore_wait(barrier, 1)
            side_copy.start()

    with scope("e_side"):
        @pl.when(core == 1)
        def _():
            side_copy.wait_recv()
            part = (side + side_recv[...]).astype(jnp.bfloat16)
            part_send[...] = part
            for n in range(7):
                part_copy(n).start()
            go(0)
            part_recv[lax.div(bi, 2)] = part

            def announce(first, last):
                def one(q):
                    @pl.when(q != sj)
                    def _():
                        pl.semaphore_signal(late_sem, inc=1, device_id=(bi, q), device_id_type=MESH)

                loop(first, last, one)

            @pl.when(late)
            def _():
                announce(0, 16)

        @pl.when(core == 0)
        def _():
            pl.semaphore_wait(go_sem.at[0], 1)

    with scope("e_send1"):
        @pl.when(late)
        def _():
            send_raw(3)
            send_raw(2)

        @pl.when(early)
        def _():
            send_raw(1)
            send_raw(0)

        raw_recv[sj] = raw_send[own]

        @pl.when(first_row)
        def _():
            more_recv[sj] = raw_send[own + 4]

    loads[1].wait()
    loads[2].wait()
    row8 = iota((8, 256), 0)
    odd32 = iota((32, 256), 0) * 2 + 1
    coarse = row8 * 8 + 4
    fine = jnp.where(row8 == 0, 1, 3)

    def tables(j, f, tabc, tabt, tabr):
        lanes = pl.ds(pl.multiple_of(j * 256, 256), 256)
        cx = cov[0:1, lanes] * f
        cy = cov[1:2, lanes] * f
        c, s = cos_sin(coarse * cx)
        tabc[0, :, lanes] = c
        tabc[1, :, lanes] = s
        c, s = cos_sin(jnp.where(row8 < 2, fine * cx, jnp.broadcast_to(cx + cy, (8, 256))))
        tabr[0, :, lanes] = c
        tabr[1, :, lanes] = s
        cyt, syt = cos_sin(odd32 * cy)
        cols = []
        for trig in range(2):
            for tab in (cyt, -syt):
                for k in range(2):
                    cols.append(tabr[trig, k : k + 1, lanes] * tab)
        tabt[lanes, :] = jnp.concatenate(cols, 0).astype(jnp.bfloat16).T

    with scope("f_tables"):
        loop(0, 16, lambda j: tables(j, f1, tabc, tabt, tabr))

        @pl.when(first_row)
        def _():
            loop(0, 16, lambda j: tables(j, f1 + 4, tabc2, tabt2, tabr2))

    @pl.when(core == 1)
    def _():
        with scope("g_partwait"):
            wait_all(part_recv, 7, part_rs)
        with scope("h_total"):
            total = part_recv[0].astype(jnp.float32)
            for p in range(1, 8):
                total = total + part_recv[p].astype(jnp.float32)
            total = total.astype(jnp.bfloat16)
            tot_send[...] = total

            @pl.when(late)
            def _():
                send_tot(3)
                send_tot(2)

            @pl.when(early)
            def _():
                send_tot(1)
                send_tot(0)

            tot_recv[sj] = total

    with scope("i_pick"):
        beams = pl.ds(pl.multiple_of(pair * 1024, 1024), 1024)
        sx = slv[0:1, beams]
        sy = slv[1:2, beams]
        u = sx + 32
        m = lax.shift_right_arithmetic(u, 2)
        f = u & 3
        cpos = m >= 8
        fpos = f >= 2
        ypos = sy >= 0
        cidx = jnp.where(cpos, m - 8, 7 - m)
        fidx = jnp.where(fpos, f - 2, 1 - f)
        ky = jnp.where(ypos, sy, -1 - sy)
        c01 = jnp.where(cpos, 1, 0)
        rel = jnp.where(c01 == jnp.where(fpos, 1, 0), 0, 1)
        diff = jnp.where(c01 == jnp.where(ypos, 1, 0), 0, 1)
        pick_row = (rel * 2 + 1 - c01) * 8 + cidx
        pick_col = diff * 64 + fidx * 32 + ky
    with scope("i_late"):
        @pl.when(early & (core == 1))
        def _():
            pl.semaphore_wait(late_sem, 8)
            go(1)
            send_tot(2)
            send_tot(3)

        @pl.when(late & (core == 1))
        def _():
            pl.semaphore_wait(late_sem, 7)
            go(1)
            send_tot(1)
            send_tot(0)

        @pl.when(core == 0)
        def _():
            pl.semaphore_wait(go_sem.at[1], 1)

        @pl.when(early)
        def _():
            send_raw(2)
            send_raw(3)

        @pl.when(late)
        def _():
            send_raw(1)
            send_raw(0)

    first = (raw_recv, tabc, tabt, tabr, xrot, wbuf, accum)
    second = (more_recv, tabc2, tabt2, tabr2, xrot2, wbuf2, accum2)

    def rotate(n, bufs):
        raw_recv, tabc, tabt, tabr, xrot, wbuf, accum = bufs

        def block(y):
            j = rows[n] * 4 + y
            lanes = pl.ds(pl.multiple_of(j * 256, 256), 256)
            raw = raw_recv[j].astype(jnp.float32)
            re = jnp.concatenate([raw[:8], raw[16:24]], 1)
            im = jnp.concatenate([raw[8:16], raw[24:]], 1)
            c = tabr[0, 2:3, lanes]
            s = tabr[1, 2:3, lanes]
            xrot[0:8, lanes] = re * c - im * s
            xrot[8:16, lanes] = im * c + re * s

        loop(0, 4, block)

    def scales(n):
        parts = []
        for y in range(4):
            total = tot_recv[rows[n] * 4 + y].astype(jnp.float32)
            parts += [total[:8], total[8:]]
        return lax.rsqrt(jnp.concatenate(parts, 1) * (1.0 / 256) + epsilon)

    def amplitudes(n, inv, bufs):
        raw_recv, tabc, tabt, tabr, xrot, wbuf, accum = bufs
        lanes = pl.ds(pl.multiple_of(rows[n] * 1024, 1024), 1024)
        at = slice(n * 1024, n * 1024 + 1024)
        wbuf[0:8, at] = xrot[0:8, lanes] * inv
        wbuf[8:16, at] = xrot[8:16, lanes] * inv
        v = []
        for trig in range(2):
            tab = tabc[trig, :, lanes]
            for row in range(16):
                v.append(wbuf[row : row + 1, at] * tab)
        acc = jnp.dot(
            jnp.concatenate(v, 0).astype(jnp.bfloat16), tabt[lanes, :], preferred_element_type=jnp.float32
        )
        if n == 0:
            accum[...] = acc
        elif n == 1:
            accum[...] += acc
        return acc

    def powers(acc):
        cc, cs, sc, ss = acc[:128, :128], acc[:128, 128:], acc[128:, :128], acc[128:, 128:]
        grid = []

        def seg_sum(a):
            a = a * a
            total = a[:8]
            for g in range(1, 8):
                total = total + a[8 * g : 8 * g + 8]
            return total

        for x, y in ((cc - ss, sc + cs), (cc + ss, sc - cs)):
            y = pltpu.roll(y, 64, 1)
            plus, minus = x + y, x - y
            turn_plus, turn_minus = pltpu.roll(plus[64:], 64, 1), pltpu.roll(minus[64:], 64, 1)
            grid.append(seg_sum(plus[:64] - turn_minus) + pltpu.roll(seg_sum(minus[:64] + turn_plus), 64, 1))
            grid.append(seg_sum(plus[:64] + turn_minus) + pltpu.roll(seg_sum(minus[:64] - turn_plus), 64, 1))
        return jnp.concatenate(grid, 0) * (1.0 / 32768)

    def pick(grid, tiles, base):
        row = iota((8, 128), 0)
        for n in range(tiles):
            at = slice(128 * n, 128 * n + 128)
            col = jnp.broadcast_to(pick_col[:, at], (8, 128))
            hit = jnp.broadcast_to(pick_row[:, at], (8, 128))
            total = jnp.zeros((8, 128), jnp.float32)
            for k in range(4):
                values = jnp.take_along_axis(grid[8 * k : 8 * k + 8], col, axis=1)
                total = total + jnp.where(row + 8 * k == hit, values, 0.0)
            pow_send[base + n] = jnp.sum(total, 0, keepdims=True)

    for n in range(4):
        if n % 2 == 0:
            with scope("j_rawwait"):
                @pl.when(first_row)
                def _(n=n):
                    wait_all(raw_recv, 14 + n, raw_rs.at[n // 2])

                @pl.when(next_row | plain)
                def _(n=n):
                    wait_all(raw_recv, 7 + n // 2, raw_rs.at[n // 2])

            with scope("k_rotate"):
                rotate(n, first)
                rotate(n + 1, first)

                @pl.when(first_row)
                def _(n=n):
                    rotate(n, second)
                    rotate(n + 1, second)

        def take_totals(n):
            @pl.when(core == 0)
            def _():
                wait_all(tot_recv, 4, tot_rs.at[n])

            @pl.when(core == 1)
            def _():
                wait_all(tot_recv, 4 if n else 3, tot_rs.at[n])
                forward_copy(n).start()

        with scope("l_totwait%d" % n):
            if n == 2:
                @pl.when(pz == 0)
                def _():
                    take_totals(3)

            if n == 3:
                @pl.when(pz > 0)
                def _():
                    take_totals(3)
            else:
                take_totals(n)

        with scope("m_main"):
            if n < 2:
                @pl.when(first_row)
                def _(n=n):
                    inv = scales(n)
                    amplitudes(n, inv, first)
                    amplitudes(n, inv, second)

                @pl.when(next_row | plain)
                def _(n=n):
                    amplitudes(n, scales(n), first)
            elif n == 2:
                @pl.when(first_row)
                def _():
                    inv = [scales(2), scales(3)]
                    pick(powers(amplitudes(2, inv[0], second) + amplitudes(3, inv[1], second) + accum2[...]), 4, 8)
                    pick(powers(amplitudes(2, inv[0], first) + amplitudes(3, inv[1], first) + accum[...]), 8, 0)

                @pl.when((pz == 0) & (pl_lo == 1))
                def _():
                    pick(powers(amplitudes(2, scales(2), first) + amplitudes(3, scales(3), first) + accum[...]), 8, 0)

                @pl.when(pz > 0)
                def _():
                    accum[...] += amplitudes(2, scales(2), first)
            else:
                @pl.when(pz > 0)
                def _():
                    pick(powers(amplitudes(3, scales(3), first) + accum[...]), 8, 0)

    with scope("o_powsend"):
        @pl.when(first_row)
        def _():
            for dy in (2, 1, 3):
                m = lax.rem(own + dy, 4)
                pow_copy(8 + m, m, own + 4).start()
                pow_copy(m, m, own).start()
            for y in range(4, 8):
                pow_copy(y, y, own).start()
            pow_recv[own + 4] = pow_send[8 + own]

        @pl.when(next_row)
        def _():
            for dy in (2, 1, 3):
                m = 4 + lax.rem(own + dy, 4)
                pow_copy(m, m, own).start()

        @pl.when(plain)
        def _():
            for d in range(7, 0, -1):
                m = lax.rem(own + d, 8)
                pow_copy(m, m, own).start()

        pow_recv[own] = pow_send[own]

    with scope("p_sendwait"):
        @pl.when(core == 0)
        def _():
            side_copy.wait_send()

        @pl.when(core == 1)
        def _():
            wait_all(part_recv, 7, part_ss)
            wait_all(tot_recv, 15, tot_ss)
            wait_all(tot_recv, 16, forward_ss)

        wait_all(raw_recv, 15, raw_ss)

        @pl.when(first_row)
        def _():
            wait_all(more_recv, 3, more_ss)

        @pl.when((pz > 0) & (pl_lo == 0))
        def _():
            wait_all(more_recv, 4, more_ss)

    with scope("q_powwait"):
        @pl.when(first_row)
        def _():
            wait_all(pow_send, 6, pow_rs)

        @pl.when(next_row | plain)
        def _():
            wait_all(pow_send, 7, pow_rs)

    with scope("r_end"):
        for b in range(8):
            out_ref[b : b + 1, :] = pow_recv[b]
        for row, count in ((first_row, 10), (next_row, 3), (plain, 7)):
            @pl.when(row)
            def _(count=count):
                wait_all(pow_send, count, pow_ss)


def local(spectra, coords, slowness):
    f32, bf16, i32 = jnp.float32, jnp.bfloat16, jnp.int32
    dma = pltpu.SemaphoreType.DMA
    return pl.pallas_call(
        kernel,
        out_shape=jax.ShapeDtypeStruct((8, 128), f32),
        in_specs=[pl.BlockSpec(memory_space=pl.ANY)] * 3,
        out_specs=pl.BlockSpec(memory_space=pltpu.VMEM),
        scratch_shapes=[
            pltpu.VMEM((2, 8, 8, 256), bf16),
            pltpu.VMEM((2, 4096), i32),
            pltpu.VMEM((2, 2048), i32),
            pltpu.VMEM((8, 32, 128), bf16),
            pltpu.VMEM((16, 32, 128), bf16),
            pltpu.VMEM((16, 32, 128), bf16),
            pltpu.VMEM((16, 128), f32),
            pltpu.VMEM((16, 128), f32),
            pltpu.VMEM((16, 128), bf16),
            pltpu.VMEM((8, 16, 128), bf16),
            pltpu.VMEM((16, 128), bf16),
            pltpu.VMEM((16, 16, 128), bf16),
            pltpu.VMEM((12, 1, 128), f32),
            pltpu.VMEM((8, 1, 128), f32),
            pltpu.VMEM((2, 8, 4096), f32),
            pltpu.VMEM((4096, 256), bf16),
            pltpu.VMEM((2, 8, 4096), f32),
            pltpu.VMEM((16, 4096), f32),
            pltpu.VMEM((16, 4096), f32),
            pltpu.VMEM((256, 256), f32),
            pltpu.VMEM((2, 8, 4096), f32),
            pltpu.VMEM((4096, 256), bf16),
            pltpu.VMEM((2, 8, 4096), f32),
            pltpu.VMEM((16, 4096), f32),
            pltpu.VMEM((16, 4096), f32),
            pltpu.VMEM((256, 256), f32),
            dma((3,)),
            pltpu.SemaphoreType.REGULAR,
            pltpu.SemaphoreType.REGULAR((2,)),
            dma, dma,
            dma, dma, dma, dma, dma((2,)), dma, dma((4,)), dma, dma, dma,
        ],
        compiler_params=pltpu.CompilerParams(
            collective_id=0, has_side_effects=True, vmem_limit_bytes=56540000
        ),
    )(spectra, coords, slowness)


def solution(mesh):
    in_specs = (P(None, "bins", None, "sta"), P(), P())
    out_specs = P("bins", "sta")
    return jax.shard_map(local, mesh=mesh, in_specs=in_specs, out_specs=out_specs, check_vma=False)
```

```python
import jax
import jax.numpy as jnp
import numpy as np
from jax import lax
from jax.experimental import pallas as pl
from jax.experimental.pallas import tpu as pltpu
from jax.sharding import PartitionSpec as P

MESH = pl.DeviceIdType.MESH
epsilon = 1e-06
scope = jax.named_scope

FAR_Y = (2, 1, 3, 0)
FAR_BINS = sorted(((dx, dl) for dx in range(4) for dl in range(2)), key=lambda o: -min(o[0], 4 - o[0]) - o[1])


def cheb_fit(fn, degree):
    nodes = np.cos(np.pi * (np.arange(4001) + 0.5) / 4001)
    u = (nodes + 1.0) / 2.0
    return np.polynomial.chebyshev.Chebyshev.fit(u, fn(u), degree, domain=[0, 1]).convert(
        kind=np.polynomial.Polynomial
    ).coef


COS = [float(c) for c in cheb_fit(lambda u: np.cos(np.pi * np.sqrt(u)), 7)]
SIN = [float(c) for c in cheb_fit(lambda u: np.pi * np.sinc(np.sqrt(u)), 6)]


def horner(coefs, u):
    acc = jnp.full_like(u, coefs[-1])
    for c in coefs[-2::-1]:
        acc = acc * u + c
    return acc


def cos_sin(index):
    t = lax.shift_right_arithmetic(lax.shift_left(index, 11), 11).astype(jnp.float32) * (1.0 / 1048576)
    u = t * t
    return horner(COS, u), horner(SIN, u) * t


def iota(shape, dim):
    return lax.broadcasted_iota(jnp.int32, shape, dim)


def kernel(
    x_hbm, co_hbm, sl_hbm, out_ref,
    xv, cov, slv, raw_send, raw_recv, more_recv, side_send, side_recv, part_send, part_recv, tot_send, tot_recv, pow_send, pow_recv,
    tabc, tabt, tabr, xrot, wbuf, accum,
    tabc2, tabt2, tabr2, xrot2, wbuf2, accum2,
    in_sem, late_sem, go_sem, side_ss, side_rs, part_ss, part_rs, raw_ss, more_ss, raw_rs, tot_ss, tot_rs, forward_ss, pow_ss, pow_rs,
):
    bi = lax.axis_index("bins")
    sj = lax.axis_index("sta")
    core = lax.rem(bi, 2)
    chip = bi - core
    px = lax.div(bi, 4)
    pl_lo = lax.rem(lax.div(bi, 2), 2)
    pz = lax.div(sj, 4)
    py = lax.rem(sj, 4)
    pair = lax.div(sj, 8)
    own = lax.rem(sj, 8)
    f1 = bi * 8 + own + 1

    early = pz < 2
    late = pz >= 2
    first_row = (pz == 0) & (pl_lo == 0)
    next_row = (pz == 1) & (pl_lo == 0)
    plain = (pz >= 2) | (pl_lo == 1)
    rows = (pz, pz + 1 - 2 * lax.rem(pz, 2), 3 - pz, lax.rem(pz + 2, 4))

    def sta_at(n, dy):
        return rows[n] * 4 + lax.rem(py + dy, 4)

    def chip_at(o):
        return lax.rem(px + o[0], 4) * 4 + lax.rem(pl_lo + o[1], 2) * 2

    loads = [
        pltpu.make_async_copy(src, dst, in_sem.at[n])
        for n, (src, dst) in enumerate(((x_hbm, xv), (co_hbm, cov), (sl_hbm, slv)))
    ]
    for load in loads:
        load.start()

    barrier = pltpu.get_barrier_semaphore()

    def greet(b, s):
        pl.semaphore_signal(barrier, inc=1, device_id=(b, s), device_id_type=MESH)

    def loop(lo, hi, body):
        lax.fori_loop(lo, hi, lambda d, c: (body(d), c)[1], 0)

    with scope("a_greet"):
        @pl.when(core == 1)
        def _():
            greet(chip, sj)
            for o in FAR_BINS[:7]:
                greet(chip_at(o) + 1, sj)

            @pl.when(early)
            def _():
                loop(1, 16, lambda d: greet(bi, lax.rem(sj + d, 16)))

            @pl.when(late)
            def _():
                loop(1, 8, lambda d: greet(bi, 8 + lax.rem(sj + d, 8)))

        @pl.when(early & (core == 0))
        def _():
            loop(1, 16, lambda d: greet(chip + 1, lax.rem(sj + d, 16)))

    with scope("b_xwait"):
        loads[0].wait()

    with scope("c_sumsq"):
        sq = jnp.zeros((8, 256), jnp.float32)
        for b in range(8):
            re = xv[0, b].astype(jnp.float32)
            im = xv[1, b].astype(jnp.float32)
            sq = sq + (re * re + im * im)
            raw_send[b] = jnp.concatenate(
                [re[:, :128], im[:, :128], re[:, 128:], im[:, 128:]], 0
            ).astype(jnp.bfloat16)
        side = jnp.concatenate([sq[:, :128], sq[:, 128:]], 0)
        side_send[...] = side

    side_copy = pltpu.make_async_remote_copy(
        src_ref=side_send, dst_ref=side_recv, send_sem=side_ss, recv_sem=side_rs,
        device_id=(chip + 1, sj), device_id_type=MESH,
    )

    def go(n):
        pl.semaphore_signal(go_sem.at[n], inc=1, device_id=(chip, sj), device_id_type=MESH)

    def part_copy(n):
        return pltpu.make_async_remote_copy(
            src_ref=part_send, dst_ref=part_recv.at[lax.div(bi, 2)],
            send_sem=part_ss, recv_sem=part_rs,
            device_id=(chip_at(FAR_BINS[n]) + 1, sj), device_id_type=MESH,
        )

    def raw_copy(n, dy):
        q = sta_at(n, dy)
        return pltpu.make_async_remote_copy(
            src_ref=raw_send.at[lax.rem(q, 8)], dst_ref=raw_recv.at[sj],
            send_sem=raw_ss, recv_sem=raw_rs.at[n // 2],
            device_id=(bi, q), device_id_type=MESH,
        )

    def tot_copy(n, dy):
        return pltpu.make_async_remote_copy(
            src_ref=tot_send, dst_ref=tot_recv.at[sj],
            send_sem=tot_ss, recv_sem=tot_rs.at[n],
            device_id=(bi, sta_at(n, dy)), device_id_type=MESH,
        )

    def forward_copy(n):
        block = tot_recv.at[pl.ds(rows[n] * 4, 4)]
        return pltpu.make_async_remote_copy(
            src_ref=block, dst_ref=block, send_sem=forward_ss, recv_sem=tot_rs.at[n],
            device_id=(chip, sj), device_id_type=MESH,
        )

    def more_copy(n, dy):
        q = sta_at(n, dy)
        return pltpu.make_async_remote_copy(
            src_ref=raw_send.at[lax.rem(q, 4) + 4], dst_ref=more_recv.at[sj],
            send_sem=more_ss, recv_sem=raw_rs.at[n // 2],
            device_id=(bi, q), device_id_type=MESH,
        )

    def send_raw(n):
        for dy in FAR_Y:
            if (n, dy) != (0, 0):
                raw_copy(n, dy).start()

        @pl.when((pz == (0, 1, 3, 2)[n]) & (pl_lo == 0))
        def _():
            for dy in FAR_Y:
                if (n, dy) != (0, 0):
                    more_copy(n, dy).start()

    def send_tot(n):
        for dy in FAR_Y:
            if (n, dy) != (0, 0):
                tot_copy(n, dy).start()

    def pow_copy(tile, m, slot):
        return pltpu.make_async_remote_copy(
            src_ref=pow_send.at[tile], dst_ref=pow_recv.at[slot],
            send_sem=pow_ss, recv_sem=pow_rs,
            device_id=(bi, pair * 8 + m), device_id_type=MESH,
        )

    def wait_all(buf, count, sem):
        blocks = buf.at[pl.ds(0, count)]
        pltpu.make_async_copy(blocks, blocks, sem).wait()

    with scope("d_barrier"):
        @pl.when(early & (core == 1))
        def _():
            pl.semaphore_wait(barrier, 21)

        @pl.when(late & (core == 1))
        def _():
            pl.semaphore_wait(barrier, 30)

        @pl.when(core == 0)
        def _():
            pl.semaphore_wait(barrier, 1)
            side_copy.start()

    with scope("e_side"):
        @pl.when(core == 1)
        def _():
            side_copy.wait_recv()
            part = (side + side_recv[...]).astype(jnp.bfloat16)
            part_send[...] = part
            for n in range(7):
                part_copy(n).start()
            go(0)
            part_recv[lax.div(bi, 2)] = part

            def announce(first, last):
                def one(q):
                    @pl.when(q != sj)
                    def _():
                        pl.semaphore_signal(late_sem, inc=1, device_id=(bi, q), device_id_type=MESH)

                loop(first, last, one)

            @pl.when(late)
            def _():
                announce(0, 16)

        @pl.when(core == 0)
        def _():
            pl.semaphore_wait(go_sem.at[0], 1)

    with scope("e_send1"):
        @pl.when(late)
        def _():
            send_raw(3)
            send_raw(2)

        @pl.when(early)
        def _():
            send_raw(1)
            send_raw(0)

        raw_recv[sj] = raw_send[own]

        @pl.when(first_row)
        def _():
            more_recv[sj] = raw_send[own + 4]

    loads[1].wait()
    loads[2].wait()
    row8 = iota((8, 256), 0)
    odd32 = iota((32, 256), 0) * 2 + 1
    coarse = row8 * 8 + 4
    fine = jnp.where(row8 == 0, 1, 3)

    def tables(j, f, tabc, tabt, tabr):
        lanes = pl.ds(pl.multiple_of(j * 256, 256), 256)
        cx = cov[0:1, lanes] * f
        cy = cov[1:2, lanes] * f
        c, s = cos_sin(coarse * cx)
        tabc[0, :, lanes] = c
        tabc[1, :, lanes] = s
        c, s = cos_sin(jnp.where(row8 < 2, fine * cx, jnp.broadcast_to(cx + cy, (8, 256))))
        tabr[0, :, lanes] = c
        tabr[1, :, lanes] = s
        cyt, syt = cos_sin(odd32 * cy)
        cols = []
        for trig in range(2):
            for tab in (cyt, -syt):
                for k in range(2):
                    cols.append(tabr[trig, k : k + 1, lanes] * tab)
        tabt[lanes, :] = jnp.concatenate(cols, 0).astype(jnp.bfloat16).T

    with scope("f_tables"):
        loop(0, 16, lambda j: tables(j, f1, tabc, tabt, tabr))

        @pl.when(first_row)
        def _():
            loop(0, 16, lambda j: tables(j, f1 + 4, tabc2, tabt2, tabr2))

    @pl.when(core == 1)
    def _():
        with scope("g_partwait"):
            wait_all(part_recv, 7, part_rs)
        with scope("h_total"):
            total = part_recv[0].astype(jnp.float32)
            for p in range(1, 8):
                total = total + part_recv[p].astype(jnp.float32)
            total = total.astype(jnp.bfloat16)
            tot_send[...] = total

            @pl.when(late)
            def _():
                send_tot(3)
                send_tot(2)

            @pl.when(early)
            def _():
                send_tot(1)
                send_tot(0)

            tot_recv[sj] = total

    with scope("i_pick"):
        beams = pl.ds(pl.multiple_of(pair * 1024, 1024), 1024)
        sx = slv[0:1, beams]
        sy = slv[1:2, beams]
        u = sx + 32
        m = lax.shift_right_arithmetic(u, 2)
        f = u & 3
        cpos = m >= 8
        fpos = f >= 2
        ypos = sy >= 0
        cidx = jnp.where(cpos, m - 8, 7 - m)
        fidx = jnp.where(fpos, f - 2, 1 - f)
        ky = jnp.where(ypos, sy, -1 - sy)
        c01 = jnp.where(cpos, 1, 0)
        rel = jnp.where(c01 == jnp.where(fpos, 1, 0), 0, 1)
        diff = jnp.where(c01 == jnp.where(ypos, 1, 0), 0, 1)
        pick_row = (rel * 2 + 1 - c01) * 8 + cidx
        pick_col = diff * 64 + fidx * 32 + ky
    with scope("i_late"):
        @pl.when(early & (core == 1))
        def _():
            pl.semaphore_wait(late_sem, 8)
            go(1)
            send_tot(2)
            send_tot(3)

        @pl.when(late & (core == 1))
        def _():
            pl.semaphore_wait(late_sem, 7)
            go(1)
            send_tot(1)
            send_tot(0)

        @pl.when(core == 0)
        def _():
            pl.semaphore_wait(go_sem.at[1], 1)

        @pl.when(early)
        def _():
            send_raw(2)
            send_raw(3)

        @pl.when(late)
        def _():
            send_raw(1)
            send_raw(0)

    first = (raw_recv, tabc, tabt, tabr, xrot, wbuf, accum)
    second = (more_recv, tabc2, tabt2, tabr2, xrot2, wbuf2, accum2)

    def rotate(n, bufs):
        raw_recv, tabc, tabt, tabr, xrot, wbuf, accum = bufs

        def block(y):
            j = rows[n] * 4 + y
            lanes = pl.ds(pl.multiple_of(j * 256, 256), 256)
            raw = raw_recv[j].astype(jnp.float32)
            re = jnp.concatenate([raw[:8], raw[16:24]], 1)
            im = jnp.concatenate([raw[8:16], raw[24:]], 1)
            c = tabr[0, 2:3, lanes]
            s = tabr[1, 2:3, lanes]
            xrot[0:8, lanes] = re * c - im * s
            xrot[8:16, lanes] = im * c + re * s

        loop(0, 4, block)

    def scales(n):
        parts = []
        for y in range(4):
            total = tot_recv[rows[n] * 4 + y].astype(jnp.float32)
            parts += [total[:8], total[8:]]
        return lax.rsqrt(jnp.concatenate(parts, 1) * (1.0 / 256) + epsilon)

    def amplitudes(n, inv, bufs):
        raw_recv, tabc, tabt, tabr, xrot, wbuf, accum = bufs
        lanes = pl.ds(pl.multiple_of(rows[n] * 1024, 1024), 1024)
        at = slice(n * 1024, n * 1024 + 1024)
        wbuf[0:8, at] = xrot[0:8, lanes] * inv
        wbuf[8:16, at] = xrot[8:16, lanes] * inv
        v = []
        for trig in range(2):
            tab = tabc[trig, :, lanes]
            for row in range(16):
                v.append(wbuf[row : row + 1, at] * tab)
        acc = jnp.dot(
            jnp.concatenate(v, 0).astype(jnp.bfloat16), tabt[lanes, :], preferred_element_type=jnp.float32
        )
        return acc if n == 0 else acc + accum[...]

    def powers(acc):
        cc, cs, sc, ss = acc[:128, :128], acc[:128, 128:], acc[128:, :128], acc[128:, 128:]
        grid = []

        def seg_sum(a):
            a = a * a
            total = a[:8]
            for g in range(1, 8):
                total = total + a[8 * g : 8 * g + 8]
            return total

        for x, y in ((cc - ss, sc + cs), (cc + ss, sc - cs)):
            y = pltpu.roll(y, 64, 1)
            plus, minus = x + y, x - y
            turn_plus, turn_minus = pltpu.roll(plus[64:], 64, 1), pltpu.roll(minus[64:], 64, 1)
            grid.append(seg_sum(plus[:64] - turn_minus) + pltpu.roll(seg_sum(minus[:64] + turn_plus), 64, 1))
            grid.append(seg_sum(plus[:64] + turn_minus) + pltpu.roll(seg_sum(minus[:64] - turn_plus), 64, 1))
        return jnp.concatenate(grid, 0) * (1.0 / 32768)

    def pick(grid, tiles, base):
        row = iota((8, 128), 0)
        for n in range(tiles):
            at = slice(128 * n, 128 * n + 128)
            col = jnp.broadcast_to(pick_col[:, at], (8, 128))
            hit = jnp.broadcast_to(pick_row[:, at], (8, 128))
            total = jnp.zeros((8, 128), jnp.float32)
            for k in range(4):
                values = jnp.take_along_axis(grid[8 * k : 8 * k + 8], col, axis=1)
                total = total + jnp.where(row + 8 * k == hit, values, 0.0)
            pow_send[base + n] = jnp.sum(total, 0, keepdims=True)

    for n in range(4):
        if n % 2 == 0:
            with scope("j_rawwait"):
                @pl.when(first_row)
                def _(n=n):
                    wait_all(raw_recv, 14 + n, raw_rs.at[n // 2])

                @pl.when(next_row | plain)
                def _(n=n):
                    wait_all(raw_recv, 7 + n // 2, raw_rs.at[n // 2])

            with scope("k_rotate"):
                rotate(n, first)
                rotate(n + 1, first)

                @pl.when(first_row)
                def _(n=n):
                    rotate(n, second)
                    rotate(n + 1, second)

        def take_totals(n):
            @pl.when(core == 0)
            def _():
                wait_all(tot_recv, 4, tot_rs.at[n])

            @pl.when(core == 1)
            def _():
                wait_all(tot_recv, 4 if n else 3, tot_rs.at[n])
                forward_copy(n).start()

        with scope("l_totwait%d" % n):
            if n < 2:
                take_totals(n)
            else:
                @pl.when(pz == 0)
                def _(n=n):
                    take_totals(5 - n)

                @pl.when(pz > 0)
                def _(n=n):
                    take_totals(n)

        with scope("m_main"):
            at_row0 = 5 - n if n > 1 else n

            @pl.when(first_row)
            def _(n=n):
                inv = scales(at_row0)
                acc2 = amplitudes(at_row0, inv, second)
                acc = amplitudes(at_row0, inv, first)
                if n == 3:
                    pick(powers(acc2), 4, 8)
                    pick(powers(acc), 8, 0)
                else:
                    accum2[...] = acc2
                    accum[...] = acc

            for row, k in ((pz == 0) & (pl_lo == 1), at_row0), (pz > 0, n):
                @pl.when(row)
                def _(n=n, k=k):
                    acc = amplitudes(k, scales(k), first)
                    if n == 3:
                        pick(powers(acc), 8, 0)
                    else:
                        accum[...] = acc

    with scope("o_powsend"):
        @pl.when(first_row)
        def _():
            for dy in (2, 1, 3):
                m = lax.rem(own + dy, 4)
                pow_copy(8 + m, m, own + 4).start()
                pow_copy(m, m, own).start()
            for y in range(4, 8):
                pow_copy(y, y, own).start()
            pow_recv[own + 4] = pow_send[8 + own]

        @pl.when(next_row)
        def _():
            for dy in (2, 1, 3):
                m = 4 + lax.rem(own + dy, 4)
                pow_copy(m, m, own).start()

        @pl.when(plain)
        def _():
            for d in range(7, 0, -1):
                m = lax.rem(own + d, 8)
                pow_copy(m, m, own).start()

        pow_recv[own] = pow_send[own]

    with scope("p_sendwait"):
        @pl.when(core == 0)
        def _():
            side_copy.wait_send()

        @pl.when(core == 1)
        def _():
            wait_all(part_recv, 7, part_ss)
            wait_all(tot_recv, 15, tot_ss)
            wait_all(tot_recv, 16, forward_ss)

        wait_all(raw_recv, 15, raw_ss)

        @pl.when(first_row)
        def _():
            wait_all(more_recv, 3, more_ss)

        @pl.when((pz > 0) & (pl_lo == 0))
        def _():
            wait_all(more_recv, 4, more_ss)

    with scope("q_powwait"):
        @pl.when(first_row)
        def _():
            wait_all(pow_send, 6, pow_rs)

        @pl.when(next_row | plain)
        def _():
            wait_all(pow_send, 7, pow_rs)

    with scope("r_end"):
        for b in range(8):
            out_ref[b : b + 1, :] = pow_recv[b]
        for row, count in ((first_row, 10), (next_row, 3), (plain, 7)):
            @pl.when(row)
            def _(count=count):
                wait_all(pow_send, count, pow_ss)


def local(spectra, coords, slowness):
    f32, bf16, i32 = jnp.float32, jnp.bfloat16, jnp.int32
    dma = pltpu.SemaphoreType.DMA
    return pl.pallas_call(
        kernel,
        out_shape=jax.ShapeDtypeStruct((8, 128), f32),
        in_specs=[pl.BlockSpec(memory_space=pl.ANY)] * 3,
        out_specs=pl.BlockSpec(memory_space=pltpu.VMEM),
        scratch_shapes=[
            pltpu.VMEM((2, 8, 8, 256), bf16),
            pltpu.VMEM((2, 4096), i32),
            pltpu.VMEM((2, 2048), i32),
            pltpu.VMEM((8, 32, 128), bf16),
            pltpu.VMEM((16, 32, 128), bf16),
            pltpu.VMEM((16, 32, 128), bf16),
            pltpu.VMEM((16, 128), f32),
            pltpu.VMEM((16, 128), f32),
            pltpu.VMEM((16, 128), bf16),
            pltpu.VMEM((8, 16, 128), bf16),
            pltpu.VMEM((16, 128), bf16),
            pltpu.VMEM((16, 16, 128), bf16),
            pltpu.VMEM((12, 1, 128), f32),
            pltpu.VMEM((8, 1, 128), f32),
            pltpu.VMEM((2, 8, 4096), f32),
            pltpu.VMEM((4096, 256), bf16),
            pltpu.VMEM((2, 8, 4096), f32),
            pltpu.VMEM((16, 4096), f32),
            pltpu.VMEM((16, 4096), f32),
            pltpu.VMEM((256, 256), f32),
            pltpu.VMEM((2, 8, 4096), f32),
            pltpu.VMEM((4096, 256), bf16),
            pltpu.VMEM((2, 8, 4096), f32),
            pltpu.VMEM((16, 4096), f32),
            pltpu.VMEM((16, 4096), f32),
            pltpu.VMEM((256, 256), f32),
            dma((3,)),
            pltpu.SemaphoreType.REGULAR,
            pltpu.SemaphoreType.REGULAR((2,)),
            dma, dma,
            dma, dma, dma, dma, dma((2,)), dma, dma((4,)), dma, dma, dma,
        ],
        compiler_params=pltpu.CompilerParams(
            collective_id=0, has_side_effects=True, vmem_limit_bytes=56540000
        ),
    )(spectra, coords, slowness)


def solution(mesh):
    in_specs = (P(None, "bins", None, "sta"), P(), P())
    out_specs = P("bins", "sta")
    return jax.shard_map(local, mesh=mesh, in_specs=in_specs, out_specs=out_specs, check_vma=False)
```

```python
import jax
import jax.numpy as jnp
import numpy as np
from jax import lax
from jax.experimental import pallas as pl
from jax.experimental.pallas import tpu as pltpu
from jax.sharding import PartitionSpec as P

MESH = pl.DeviceIdType.MESH
epsilon = 1e-06
scope = jax.named_scope

FAR_Y = (2, 1, 3, 0)
FAR_BINS = sorted(((dx, dl) for dx in range(4) for dl in range(2)), key=lambda o: -min(o[0], 4 - o[0]) - o[1])


def cheb_fit(fn, degree):
    nodes = np.cos(np.pi * (np.arange(4001) + 0.5) / 4001)
    u = (nodes + 1.0) / 2.0
    return np.polynomial.chebyshev.Chebyshev.fit(u, fn(u), degree, domain=[0, 1]).convert(
        kind=np.polynomial.Polynomial
    ).coef


COS = [float(c) for c in cheb_fit(lambda u: np.cos(np.pi * np.sqrt(u)), 7)]
SIN = [float(c) for c in cheb_fit(lambda u: np.pi * np.sinc(np.sqrt(u)), 6)]


def horner(coefs, u):
    acc = jnp.full_like(u, coefs[-1])
    for c in coefs[-2::-1]:
        acc = acc * u + c
    return acc


def cos_sin(index):
    t = lax.shift_right_arithmetic(lax.shift_left(index, 11), 11).astype(jnp.float32) * (1.0 / 1048576)
    u = t * t
    return horner(COS, u), horner(SIN, u) * t


def iota(shape, dim):
    return lax.broadcasted_iota(jnp.int32, shape, dim)


def kernel(
    x_hbm, co_hbm, sl_hbm, out_ref,
    xv, cov, slv, raw_send, raw_recv, more_recv, side_send, side_recv, part_send, part_recv, tot_send, tot_recv, pow_send, pow_recv,
    tabc, tabt, tabr, xrot, wbuf, accum,
    tabc2, tabt2, tabr2, xrot2, wbuf2, accum2,
    in_sem, late_sem, go_sem, side_rs, part_rs, raw_rs, tot_rs, pow_rs, sent, pow_ss,
):
    bi = lax.axis_index("bins")
    sj = lax.axis_index("sta")
    core = lax.rem(bi, 2)
    chip = bi - core
    px = lax.div(bi, 4)
    pl_lo = lax.rem(lax.div(bi, 2), 2)
    pz = lax.div(sj, 4)
    py = lax.rem(sj, 4)
    pair = lax.div(sj, 8)
    own = lax.rem(sj, 8)
    f1 = bi * 8 + own + 1

    early = pz < 2
    late = pz >= 2
    first_row = (pz == 0) & (pl_lo == 0)
    next_row = (pz == 1) & (pl_lo == 0)
    plain = (pz >= 2) | (pl_lo == 1)
    rows = (pz, pz + 1 - 2 * lax.rem(pz, 2), 3 - pz, lax.rem(pz + 2, 4))

    def sta_at(n, dy):
        return rows[n] * 4 + lax.rem(py + dy, 4)

    def chip_at(o):
        return lax.rem(px + o[0], 4) * 4 + lax.rem(pl_lo + o[1], 2) * 2

    loads = [
        pltpu.make_async_copy(src, dst, in_sem.at[n])
        for n, src, dst in ((0, x_hbm, xv), (1, co_hbm, cov), (1, sl_hbm, slv))
    ]
    for load in loads:
        load.start()

    barrier = pltpu.get_barrier_semaphore()

    def greet(b, s):
        pl.semaphore_signal(barrier, inc=1, device_id=(b, s), device_id_type=MESH)

    def loop(lo, hi, body):
        lax.fori_loop(lo, hi, lambda d, c: (body(d), c)[1], 0)

    with scope("a_greet"):
        @pl.when(core == 1)
        def _():
            greet(chip, sj)
            for o in FAR_BINS[:7]:
                greet(chip_at(o) + 1, sj)

            @pl.when(early)
            def _():
                loop(1, 16, lambda d: greet(bi, lax.rem(sj + d, 16)))

            @pl.when(late)
            def _():
                loop(1, 8, lambda d: greet(bi, 8 + lax.rem(sj + d, 8)))

        @pl.when(early & (core == 0))
        def _():
            loop(1, 16, lambda d: greet(chip + 1, lax.rem(sj + d, 16)))

    with scope("b_xwait"):
        loads[0].wait()

    with scope("c_sumsq"):
        sq = jnp.zeros((8, 256), jnp.float32)
        for b in range(8):
            re = xv[0, b].astype(jnp.float32)
            im = xv[1, b].astype(jnp.float32)
            sq = sq + (re * re + im * im)
            raw_send[b] = jnp.concatenate(
                [re[:, :128], im[:, :128], re[:, 128:], im[:, 128:]], 0
            ).astype(jnp.bfloat16)
        side = jnp.concatenate([sq[:, :128], sq[:, 128:]], 0)
        side_send[...] = side

    side_copy = pltpu.make_async_remote_copy(
        src_ref=side_send, dst_ref=side_recv, send_sem=sent, recv_sem=side_rs,
        device_id=(chip + 1, sj), device_id_type=MESH,
    )

    def go(n):
        pl.semaphore_signal(go_sem.at[n], inc=1, device_id=(chip, sj), device_id_type=MESH)

    def part_copy(n):
        return pltpu.make_async_remote_copy(
            src_ref=part_send, dst_ref=part_recv.at[lax.div(bi, 2)],
            send_sem=sent, recv_sem=part_rs,
            device_id=(chip_at(FAR_BINS[n]) + 1, sj), device_id_type=MESH,
        )

    def raw_copy(n, dy):
        q = sta_at(n, dy)
        return pltpu.make_async_remote_copy(
            src_ref=raw_send.at[lax.rem(q, 8)], dst_ref=raw_recv.at[sj],
            send_sem=sent, recv_sem=raw_rs.at[n // 2],
            device_id=(bi, q), device_id_type=MESH,
        )

    def tot_copy(n, dy):
        return pltpu.make_async_remote_copy(
            src_ref=tot_send, dst_ref=tot_recv.at[sj],
            send_sem=sent, recv_sem=tot_rs.at[n],
            device_id=(bi, sta_at(n, dy)), device_id_type=MESH,
        )

    def forward_copy(n):
        block = tot_recv.at[pl.ds(rows[n] * 4, 4)]
        return pltpu.make_async_remote_copy(
            src_ref=block, dst_ref=block, send_sem=sent, recv_sem=tot_rs.at[n],
            device_id=(chip, sj), device_id_type=MESH,
        )

    def more_copy(n, dy):
        q = sta_at(n, dy)
        return pltpu.make_async_remote_copy(
            src_ref=raw_send.at[lax.rem(q, 4) + 4], dst_ref=more_recv.at[sj],
            send_sem=sent, recv_sem=raw_rs.at[n // 2],
            device_id=(bi, q), device_id_type=MESH,
        )

    def send_raw(n):
        for dy in FAR_Y:
            if (n, dy) != (0, 0):
                raw_copy(n, dy).start()

        @pl.when((pz == (0, 1, 3, 2)[n]) & (pl_lo == 0))
        def _():
            for dy in FAR_Y:
                if (n, dy) != (0, 0):
                    more_copy(n, dy).start()

    def send_tot(n):
        for dy in FAR_Y:
            if (n, dy) != (0, 0):
                tot_copy(n, dy).start()

    def pow_copy(tile, m, slot):
        return pltpu.make_async_remote_copy(
            src_ref=pow_send.at[tile], dst_ref=pow_recv.at[slot],
            send_sem=pow_ss, recv_sem=pow_rs,
            device_id=(bi, pair * 8 + m), device_id_type=MESH,
        )

    def wait_all(buf, count, sem):
        blocks = buf.at[pl.ds(0, count)]
        pltpu.make_async_copy(blocks, blocks, sem).wait()

    with scope("d_barrier"):
        @pl.when(early & (core == 1))
        def _():
            pl.semaphore_wait(barrier, 21)

        @pl.when(late & (core == 1))
        def _():
            pl.semaphore_wait(barrier, 30)

        @pl.when(core == 0)
        def _():
            pl.semaphore_wait(barrier, 1)
            side_copy.start()

    with scope("e_side"):
        @pl.when(core == 1)
        def _():
            side_copy.wait_recv()
            part = (side + side_recv[...]).astype(jnp.bfloat16)
            part_send[...] = part
            for n in range(7):
                part_copy(n).start()
            go(0)
            part_recv[lax.div(bi, 2)] = part

            def announce(first, last):
                def one(q):
                    @pl.when(q != sj)
                    def _():
                        pl.semaphore_signal(late_sem, inc=1, device_id=(bi, q), device_id_type=MESH)

                loop(first, last, one)

            @pl.when(late)
            def _():
                announce(0, 16)

        @pl.when(core == 0)
        def _():
            pl.semaphore_wait(go_sem.at[0], 1)

    with scope("e_send1"):
        @pl.when(pz == 2)
        def _():
            send_raw(3)
            send_raw(2)

        @pl.when(pz == 3)
        def _():
            send_raw(2)
            send_raw(3)

        @pl.when(early)
        def _():
            send_raw(1)
            send_raw(0)

        raw_recv[sj] = raw_send[own]

        @pl.when(first_row)
        def _():
            more_recv[sj] = raw_send[own + 4]

    wait_all(tabt, 96, in_sem.at[1])
    row8 = iota((8, 256), 0)
    odd32 = iota((32, 256), 0) * 2 + 1
    coarse = row8 * 8 + 4
    fine = jnp.where(row8 == 0, 1, 3)

    def tables(j, f, tabc, tabt, tabr):
        lanes = pl.ds(pl.multiple_of(j * 256, 256), 256)
        cx = cov[0:1, lanes] * f
        cy = cov[1:2, lanes] * f
        c, s = cos_sin(coarse * cx)
        tabc[0, :, lanes] = c
        tabc[1, :, lanes] = s
        c, s = cos_sin(jnp.where(row8 < 2, fine * cx, jnp.broadcast_to(cx + cy, (8, 256))))
        tabr[0, :, lanes] = c
        tabr[1, :, lanes] = s
        cyt, syt = cos_sin(odd32 * cy)
        cols = []
        for trig in range(2):
            for tab in (cyt, -syt):
                for k in range(2):
                    cols.append(tabr[trig, k : k + 1, lanes] * tab)
        tabt[lanes, :] = jnp.concatenate(cols, 0).astype(jnp.bfloat16).T

    with scope("f_tables"):
        loop(0, 16, lambda j: tables(j, f1, tabc, tabt, tabr))

        @pl.when(first_row)
        def _():
            loop(0, 16, lambda j: tables(j, f1 + 4, tabc2, tabt2, tabr2))

    @pl.when(core == 1)
    def _():
        with scope("g_partwait"):
            wait_all(part_recv, 7, part_rs)
        with scope("h_total"):
            total = part_recv[0].astype(jnp.float32)
            for p in range(1, 8):
                total = total + part_recv[p].astype(jnp.float32)
            total = total.astype(jnp.bfloat16)
            tot_send[...] = total

            @pl.when(pz == 2)
            def _():
                send_tot(3)
                send_tot(2)

            @pl.when(pz == 3)
            def _():
                send_tot(2)
                send_tot(3)

            @pl.when(early)
            def _():
                send_tot(1)
                send_tot(0)

            tot_recv[sj] = total

    with scope("i_pick"):
        beams = pl.ds(pl.multiple_of(pair * 1024, 1024), 1024)
        sx = slv[0:1, beams]
        sy = slv[1:2, beams]
        u = sx + 32
        m = lax.shift_right_arithmetic(u, 2)
        f = u & 3
        cpos = m >= 8
        fpos = f >= 2
        ypos = sy >= 0
        cidx = jnp.where(cpos, m - 8, 7 - m)
        fidx = jnp.where(fpos, f - 2, 1 - f)
        ky = jnp.where(ypos, sy, -1 - sy)
        c01 = jnp.where(cpos, 1, 0)
        rel = jnp.where(c01 == jnp.where(fpos, 1, 0), 0, 1)
        diff = jnp.where(c01 == jnp.where(ypos, 1, 0), 0, 1)
        pick_row = (rel * 2 + 1 - c01) * 8 + cidx
        pick_col = diff * 64 + fidx * 32 + ky
    with scope("i_late"):
        @pl.when(early & (core == 1))
        def _():
            pl.semaphore_wait(late_sem, 8)
            go(1)
            send_tot(2)
            send_tot(3)

        @pl.when(late & (core == 1))
        def _():
            pl.semaphore_wait(late_sem, 7)
            go(1)
            send_tot(1)
            send_tot(0)

        @pl.when(core == 0)
        def _():
            pl.semaphore_wait(go_sem.at[1], 1)

        @pl.when(early)
        def _():
            send_raw(2)
            send_raw(3)

        @pl.when(late)
        def _():
            send_raw(1)
            send_raw(0)

    first = (raw_recv, tabc, tabt, tabr, xrot, wbuf, accum)
    second = (more_recv, tabc2, tabt2, tabr2, xrot2, wbuf2, accum2)

    def rotate(n, bufs):
        raw_recv, tabc, tabt, tabr, xrot, wbuf, accum = bufs

        def block(y):
            j = rows[n] * 4 + y
            lanes = pl.ds(pl.multiple_of(j * 256, 256), 256)
            raw = raw_recv[j].astype(jnp.float32)
            re = jnp.concatenate([raw[:8], raw[16:24]], 1)
            im = jnp.concatenate([raw[8:16], raw[24:]], 1)
            c = tabr[0, 2:3, lanes]
            s = tabr[1, 2:3, lanes]
            xrot[0:8, lanes] = re * c - im * s
            xrot[8:16, lanes] = im * c + re * s

        loop(0, 4, block)

    def scales(n):
        parts = []
        for y in range(4):
            total = tot_recv[rows[n] * 4 + y].astype(jnp.float32)
            parts += [total[:8], total[8:]]
        return lax.rsqrt(jnp.concatenate(parts, 1) * (1.0 / 256) + epsilon)

    def amplitudes(n, inv, bufs, onto=True):
        raw_recv, tabc, tabt, tabr, xrot, wbuf, accum = bufs
        lanes = pl.ds(pl.multiple_of(rows[n] * 1024, 1024), 1024)
        at = slice(n * 1024, n * 1024 + 1024)
        wbuf[0:8, at] = xrot[0:8, lanes] * inv
        wbuf[8:16, at] = xrot[8:16, lanes] * inv
        v = []
        for trig in range(2):
            tab = tabc[trig, :, lanes]
            for row in range(16):
                v.append(wbuf[row : row + 1, at] * tab)
        acc = jnp.dot(
            jnp.concatenate(v, 0).astype(jnp.bfloat16), tabt[lanes, :], preferred_element_type=jnp.float32
        )
        return acc + accum[...] if n and onto else acc

    def powers(acc):
        cc, cs, sc, ss = acc[:128, :128], acc[:128, 128:], acc[128:, :128], acc[128:, 128:]
        grid = []

        def seg_sum(a):
            a = a * a
            total = a[:8]
            for g in range(1, 8):
                total = total + a[8 * g : 8 * g + 8]
            return total

        for x, y in ((cc - ss, sc + cs), (cc + ss, sc - cs)):
            y = pltpu.roll(y, 64, 1)
            plus, minus = x + y, x - y
            turn_plus, turn_minus = pltpu.roll(plus[64:], 64, 1), pltpu.roll(minus[64:], 64, 1)
            grid.append(seg_sum(plus[:64] - turn_minus) + pltpu.roll(seg_sum(minus[:64] + turn_plus), 64, 1))
            grid.append(seg_sum(plus[:64] + turn_minus) + pltpu.roll(seg_sum(minus[:64] - turn_plus), 64, 1))
        return jnp.concatenate(grid, 0) * (1.0 / 32768)

    def pick(grid, first_tile, last_tile, base):
        row = iota((8, 128), 0)
        for n in range(first_tile, last_tile):
            at = slice(128 * n, 128 * n + 128)
            col = jnp.broadcast_to(pick_col[:, at], (8, 128))
            hit = jnp.broadcast_to(pick_row[:, at], (8, 128))
            total = jnp.zeros((8, 128), jnp.float32)
            for k in range(4):
                values = jnp.take_along_axis(grid[8 * k : 8 * k + 8], col, axis=1)
                total = total + jnp.where(row + 8 * k == hit, values, 0.0)
            pow_send[base + n] = jnp.sum(total, 0, keepdims=True)

    for n in range(4):
        if n % 2 == 0:
            with scope("j_rawwait"):
                @pl.when(first_row)
                def _(n=n):
                    wait_all(raw_recv, 14 + n, raw_rs.at[n // 2])

                @pl.when(next_row | plain)
                def _(n=n):
                    wait_all(raw_recv, 7 + n // 2, raw_rs.at[n // 2])

            with scope("k_rotate"):
                rotate(n, first)
                rotate(n + 1, first)

                @pl.when(first_row)
                def _(n=n):
                    rotate(n, second)
                    rotate(n + 1, second)

        def take_totals(n):
            @pl.when(core == 0)
            def _():
                wait_all(tot_recv, 4, tot_rs.at[n])

            @pl.when(core == 1)
            def _():
                wait_all(tot_recv, 4 if n else 3, tot_rs.at[n])
                forward_copy(n).start()

        with scope("l_totwait%d" % n):
            if n < 2:
                take_totals(n)
            else:
                if n == 3:
                    @pl.when(pz == 0)
                    def _():
                        take_totals(3)
                        take_totals(2)

                @pl.when(pz > 0)
                def _(n=n):
                    take_totals(n)

        with scope("m_main"):
            @pl.when(first_row)
            def _(n=n):
                if n == 2:
                    return
                inv = scales(n)
                acc2 = amplitudes(n, inv, second)
                acc = amplitudes(n, inv, first)
                if n < 2:
                    accum2[...] = acc2
                    accum[...] = acc
                    return
                inv = scales(2)
                acc2 = acc2 + amplitudes(2, inv, second, False)
                acc = acc + amplitudes(2, inv, first, False)
                pick(powers(acc2), 0, 4, 8)
                grid = powers(acc)
                pick(grid, 0, 4, 0)
                for dy in (2, 1, 3):
                    m = lax.rem(own + dy, 4)
                    pow_copy(8 + m, m, own + 4).start()
                    pow_copy(m, m, own).start()
                pick(grid, 4, 8, 0)
                for y in range(4, 8):
                    pow_copy(y, y, own).start()
                pow_recv[own + 4] = pow_send[8 + own]

            @pl.when((pz == 0) & (pl_lo == 1))
            def _(n=n):
                if n == 2:
                    return
                acc = amplitudes(n, scales(n), first)
                if n < 2:
                    accum[...] = acc
                    return
                acc = acc + amplitudes(2, scales(2), first, False)
                grid = powers(acc)
                pick(grid, 0, 4, 0)
                for dy in (2, 1, 3):
                    m = lax.rem(own + dy, 4)
                    pow_copy(m, m, own).start()
                pick(grid, 4, 8, 0)
                for y in range(4, 8):
                    pow_copy(y, y, own).start()

            @pl.when(pz > 0)
            def _(n=n):
                acc = amplitudes(n, scales(n), first)
                if n < 3:
                    accum[...] = acc
                    return
                pick(powers(acc), 0, 8, 0)

    with scope("o_powsend"):
        @pl.when(next_row)
        def _():
            for dy in (2, 1, 3):
                m = 4 + lax.rem(own + dy, 4)
                pow_copy(m, m, own).start()

        @pl.when(plain & (pz > 0))
        def _():
            for d in (4, 6, 2, 5, 3, 7, 1):
                m = lax.rem(own + d, 8)
                pow_copy(m, m, own).start()

        pow_recv[own] = pow_send[own]

    with scope("q_powwait"):
        @pl.when(first_row)
        def _():
            wait_all(pow_send, 6, pow_rs)

        @pl.when(next_row | plain)
        def _():
            wait_all(pow_send, 7, pow_rs)

    with scope("r_end"):
        for b in range(8):
            out_ref[b : b + 1, :] = pow_recv[b]
        for row, count in ((first_row, 10), (next_row, 3), (plain, 7)):
            @pl.when(row)
            def _(count=count):
                wait_all(pow_send, count, pow_ss)

        for row, count in ((first_row, 6), ((pz > 0) & (pl_lo == 0), 8), (pl_lo == 1, 0)):
            @pl.when(row & (core == 1))
            def _(count=count):
                wait_all(tabt, 8 * (68 + count), sent)

            @pl.when(row & (core == 0))
            def _(count=count):
                wait_all(tabt, 8 * (32 + count), sent)


def local(spectra, coords, slowness):
    f32, bf16, i32 = jnp.float32, jnp.bfloat16, jnp.int32
    dma = pltpu.SemaphoreType.DMA
    return pl.pallas_call(
        kernel,
        out_shape=jax.ShapeDtypeStruct((8, 128), f32),
        in_specs=[pl.BlockSpec(memory_space=pl.ANY)] * 3,
        out_specs=pl.BlockSpec(memory_space=pltpu.VMEM),
        scratch_shapes=[
            pltpu.VMEM((2, 8, 8, 256), bf16),
            pltpu.VMEM((2, 4096), i32),
            pltpu.VMEM((2, 2048), i32),
            pltpu.VMEM((8, 32, 128), bf16),
            pltpu.VMEM((16, 32, 128), bf16),
            pltpu.VMEM((16, 32, 128), bf16),
            pltpu.VMEM((16, 128), f32),
            pltpu.VMEM((16, 128), f32),
            pltpu.VMEM((16, 128), bf16),
            pltpu.VMEM((8, 16, 128), bf16),
            pltpu.VMEM((16, 128), bf16),
            pltpu.VMEM((16, 16, 128), bf16),
            pltpu.VMEM((12, 1, 128), f32),
            pltpu.VMEM((8, 1, 128), f32),
            pltpu.VMEM((2, 8, 4096), f32),
            pltpu.VMEM((4096, 256), bf16),
            pltpu.VMEM((2, 8, 4096), f32),
            pltpu.VMEM((16, 4096), f32),
            pltpu.VMEM((16, 4096), f32),
            pltpu.VMEM((256, 256), f32),
            pltpu.VMEM((2, 8, 4096), f32),
            pltpu.VMEM((4096, 256), bf16),
            pltpu.VMEM((2, 8, 4096), f32),
            pltpu.VMEM((16, 4096), f32),
            pltpu.VMEM((16, 4096), f32),
            pltpu.VMEM((256, 256), f32),
            dma((2,)),
            pltpu.SemaphoreType.REGULAR,
            pltpu.SemaphoreType.REGULAR((2,)),
            dma, dma, dma((2,)), dma((4,)), dma, dma, dma,
        ],
        compiler_params=pltpu.CompilerParams(
            collective_id=0, has_side_effects=True, vmem_limit_bytes=56540000
        ),
    )(spectra, coords, slowness)


def solution(mesh):
    in_specs = (P(None, "bins", None, "sta"), P(), P())
    out_specs = P("bins", "sta")
    return jax.shard_map(local, mesh=mesh, in_specs=in_specs, out_specs=out_specs, check_vma=False)
```
